32 devices in a mesh: ctx: 16 (over z, y, x), head: 2 (over core).
Axes of the slice: x: 2, y: 2, z: 4, core: 2. Of those that a mesh axis runs over, the one named last changes fastest.
Arguments:
- patches: bfloat16 [2048, 1280], P('ctx'), may hold values from -6 to 6
- patch_count: int32 [16], P('ctx'), may hold values from 1 to 128, as said below
- token_patch: int32 [2048], P('ctx'), may hold values from -1 to 127, as said below
- window_ids: int32 [2048], P('ctx'), may hold values from 1 to 2048, as said below
- text_embed: bfloat16 [2048, 4096], P('ctx', 'head'), may hold values from -200 to 200
- vit_norm_gain: float32 [1280], replicated, may hold values from 0.25 to 1.75
- vit_qkv: bfloat16 [1280, 3840], P(None, 'head'), may hold values from -0.15625 to 0.15625
- vit_qkv_bias: float32 [3840], P('head'), may hold values from -16 to 16
- vit_proj: bfloat16 [1280, 1280], P('head'), may hold values from -0.15625 to 0.15625
- vit_proj_bias: float32 [1280], replicated, may hold values from -1 to 1
- merge_norm_gain: float32 [1280], replicated, may hold values from 0.25 to 1.75
- merger: bfloat16 [1280, 4096], P('ctx', 'head'), may hold values from -0.15625 to 0.15625
- merger_bias: float32 [4096], P('head'), may hold values from -1 to 1
- llm_norm_gain: float32 [4096], replicated, may hold values from 0.25 to 1.75
- w_qkv: bfloat16 [4096, 6144], P('ctx', 'head'), may hold values from -0.09375 to 0.09375
- qkv_bias: float32 [6144], P('head'), may hold values from -16 to 16
Outputs:
- context: bfloat16 [2048, 4096], P('ctx', 'head')
The draws below stay inside these ranges and needn't reach their ends.
Inputs may be any that keep to these rules, and one draw needn't show every extreme that they name: `patch_count`: at most 128 live slots on one ctx index, reached by some index in every draw. `token_patch`: among the tokens of one ctx index, each live slot 0 to patch_count - 1 of that index appears exactly once; all other tokens hold -1. `window_ids`: ids never fall along the slots; a window lies within the slots of one ctx index and holds at most 64 consecutive slots; some window holds exactly 64.
All inputs are finite; a program needn't handle non-finite values.
Results may differ from the reference program's by a relative error of at most 0.012.
The reference program's roundings to bfloat16 on the way count: a program that leaves them out, or rounds other values in their place, can miss the bound.
Values may be sent and summed in bfloat16 or wider, within the bound.
No kernel may reach another device: no remote copies, remote signals or barrier semaphores. Data moves between devices by JAX's collectives and lax.ppermute only.
A program may use at most 64 MiB of HBM per device.

```python
import math
import jax
import jax.numpy as jnp
from jax import lax

DV = 1280
VH = 16
VHD = 80
KVH = 8
HD = 128
D = 4096
QH = 4
WIN = 64
TOK_DEV = 128
TOKENS = 2048
N_CTX = 16


def shard_counts(key):
    shards = TOKENS // TOK_DEV
    base = jax.random.fold_in(key, 11)
    first = jax.random.randint(jax.random.fold_in(base, 1), (shards,), 1, TOK_DEV + 1)
    second = jax.random.randint(jax.random.fold_in(base, 2), (shards,), 1, TOK_DEV + 1)
    counts = jnp.minimum(first, second)
    fullest = jax.random.randint(jax.random.fold_in(base, 3), (), 0, shards)
    return jnp.where(jnp.arange(shards) == fullest, TOK_DEV, counts).astype(jnp.int32)


def draw_patch_count(key, part):
    return shard_counts(key)


def draw_token_patch(key, part):
    shards = TOKENS // TOK_DEV
    counts = shard_counts(key)
    shard_keys = jax.random.split(jax.random.fold_in(key, 12), shards)
    orders = jax.vmap(lambda one_key: jax.random.permutation(one_key, TOK_DEV))(shard_keys)
    chosen_slots = jnp.where(orders < counts[:, None], orders, -1)
    return chosen_slots.reshape(TOKENS).astype(jnp.int32)


def draw_window_ids(key, part):
    shards = TOKENS // TOK_DEV
    base = jax.random.fold_in(key, 13)
    marks = jax.random.randint(base, (shards, TOK_DEV), 0, 12) == 0
    local = jnp.arange(TOK_DEV)
    bounds = local % WIN == 0
    chosen = jax.random.randint(jax.random.fold_in(base, 1), (), 0, shards)
    quiet = (jnp.arange(shards)[:, None] == chosen) & (local[None, :] < WIN)
    marks = marks & jnp.logical_not(quiet) | bounds[None, :]
    window_numbers = jnp.cumsum(marks.astype(jnp.int32), axis=1) + jnp.arange(shards, dtype=jnp.int32)[:, None] * TOK_DEV
    return window_numbers.reshape(TOKENS).astype(jnp.int32)


def draw_text_embed(key, part):
    base = jax.random.fold_in(key, 14)
    row_scale = jnp.exp(jax.random.uniform(jax.random.fold_in(base, 1), (TOKENS, 1), minval=0.0, maxval=math.log(10.0)))
    column_rise = jnp.exp(jnp.linspace(0.0, math.log(3.0), D))[None, :] * jax.random.uniform(jax.random.fold_in(base, 2), (1, D), minval=0.5, maxval=1.5)
    values = jax.random.truncated_normal(jax.random.fold_in(base, 5), -4.0, 4.0, (TOKENS, D)) * row_scale * column_rise
    return values.astype(jnp.float32).astype(jnp.bfloat16)


def drawn_bias(base, heads, parts, head_size):
    drawn = jax.random.truncated_normal(jax.random.fold_in(base, 1), -3.0, 3.0, (heads, parts, head_size))
    values = drawn * 0.5
    return values.reshape(heads * parts * head_size).astype(jnp.float32)


def draw_vit_qkv_bias(key, part):
    return drawn_bias(jax.random.fold_in(key, 21), VH, 3, VHD)


def draw_qkv_bias(key, part):
    return drawn_bias(jax.random.fold_in(key, 22), KVH, QH + 2, HD)


def levels(key, shape, cuts, smallest, largest):
    def one(axis_at, shards_of):
        draws = jax.random.uniform(jax.random.fold_in(jax.random.fold_in(key, 6), axis_at), (shards_of,), jnp.float32, smallest / len(cuts), largest / len(cuts))
        return jnp.repeat(jnp.exp(draws), shape[axis_at] // shards_of).reshape((-1,) + (1,) * (len(shape) - axis_at - 1))

    level = one(*cuts[0])
    for cut in cuts[1:]:
        level = level * one(*cut)
    return level


def bell_draw(stream_key, extent, width, reach, cuts=(), held_as=jnp.bfloat16):
    values = jax.random.normal(stream_key, extent, jnp.float32) * width
    if len(cuts) > 0:
        values = levels(stream_key, extent, cuts, -0.22, 0.18) * values
    return jnp.clip(values, min=-reach, max=reach).astype(held_as)


def setup_inputs(seed: int = 0) -> dict:
    streams_of = jax.random.split(jax.random.key(seed), 17)
    patches = bell_draw(streams_of[0], (TOKENS, DV), 1.0, 6.0, ((0, 16),))
    patch_count = draw_patch_count(jax.random.fold_in(streams_of[16], 71), 0)
    token_patch = draw_token_patch(jax.random.fold_in(streams_of[16], 71), 0)
    window_ids = draw_window_ids(jax.random.fold_in(streams_of[16], 71), 0)
    text_embed = draw_text_embed(jax.random.fold_in(streams_of[16], 71), 0)
    vit_norm_gain = jnp.clip(1.0 + 0.15 * jax.random.normal(streams_of[5], (DV,), jnp.float32), 0.25, 1.75)
    vit_qkv = bell_draw(streams_of[6], (DV, 3 * DV), DV ** -0.5, 0.15625, ((1, 2),))
    vit_qkv_bias = draw_vit_qkv_bias(jax.random.fold_in(streams_of[16], 71), 0)
    vit_proj = bell_draw(streams_of[8], (DV, DV), DV ** -0.5, 0.15625, ((0, 2),))
    vit_proj_bias = jnp.clip(jax.random.uniform(streams_of[9], (DV,), jnp.float32, -1.0, 1.0), -1.0, 1.0)
    merge_norm_gain = jnp.clip(1.0 + 0.15 * jax.random.normal(streams_of[10], (DV,), jnp.float32), 0.25, 1.75)
    merger = bell_draw(streams_of[11], (DV, D), DV ** -0.5, 0.15625, ((0, 16), (1, 2)))
    merger_bias = jnp.clip(jax.random.uniform(streams_of[12], (D,), jnp.float32, -1.0, 1.0) * levels(streams_of[12], (D,), ((0, 2),), -0.4, 0.0), -1.0, 1.0)
    llm_norm_gain = jnp.clip(1.0 + 0.15 * jax.random.normal(streams_of[13], (D,), jnp.float32), 0.25, 1.75)
    w_qkv = bell_draw(streams_of[14], (D, KVH * (QH + 2) * HD), D ** -0.5, 0.09375, ((0, 16), (1, 2)))
    qkv_bias = draw_qkv_bias(jax.random.fold_in(streams_of[16], 71), 0)
    return dict(patches=patches, patch_count=patch_count, token_patch=token_patch, window_ids=window_ids, text_embed=text_embed, vit_norm_gain=vit_norm_gain, vit_qkv=vit_qkv, vit_qkv_bias=vit_qkv_bias, vit_proj=vit_proj, vit_proj_bias=vit_proj_bias, merge_norm_gain=merge_norm_gain, merger=merger, merger_bias=merger_bias, llm_norm_gain=llm_norm_gain, w_qkv=w_qkv, qkv_bias=qkv_bias)


EPSILON = 1e-06
THETA = 1000000.0
MASKED = -1e+30

def rms_norm(rows, gain):
    values = rows.astype(jnp.float32)
    return (values * lax.rsqrt(lax.optimization_barrier(jnp.mean(values * values, axis=-1, keepdims=True)) + EPSILON) * gain).astype(jnp.bfloat16)

def rotate(values, positions):
    head_size = values.shape[-1]
    half = head_size // 2
    steps = jnp.arange(half, dtype=jnp.float32) * (2.0 / head_size)
    frequency = jnp.exp(-math.log(THETA) * steps)
    angle = positions.astype(jnp.float32)[:, None] * frequency[None, :]
    cosine = jnp.cos(angle)[:, None, None, :]
    sine = jnp.sin(angle)[:, None, None, :]
    first = values[..., :half]
    second = values[..., half:]
    return jnp.concatenate([first * cosine - second * sine, second * cosine + first * sine], axis=-1)

def vision_heads(normed, weight, bias, windows, count, head_size):
    slot_count = normed.shape[0]
    mixed = jnp.dot(normed, weight, preferred_element_type=jnp.float32) + bias
    heads = mixed.shape[1] // (3 * head_size)
    mixed = mixed.astype(jnp.bfloat16).reshape(slot_count, heads, 3, head_size)
    query = mixed[:, :, 0].astype(jnp.float32)
    key = mixed[:, :, 1].astype(jnp.float32)
    value = mixed[:, :, 2].astype(jnp.float32)
    scores = jnp.einsum('rhd,shd->hrs', query, key) * (1.0 / math.sqrt(head_size))
    index = jnp.arange(slot_count, dtype=jnp.int32)
    allowed = (windows[:, None] == windows[None, :]) & ((index[None, :] < count) | (index[:, None] == index[None, :]))
    scores = jnp.where(allowed[None], scores, MASKED)
    top = lax.optimization_barrier(jnp.max(scores, axis=-1, keepdims=True))
    weights = jnp.where(allowed[None], jnp.exp(scores - top), 0.0)
    total = lax.optimization_barrier(jnp.sum(weights, axis=-1))
    result = jnp.einsum('hrs,shd->rhd', weights.astype(jnp.bfloat16).astype(jnp.float32), value)
    return (result / jnp.transpose(total)[:, :, None]).astype(jnp.bfloat16).reshape(slot_count, heads * head_size)

def causal_group(inputs):
    query, key, value = inputs
    scale = 1.0 / math.sqrt(HD)
    key_wide = key.astype(jnp.float32)
    value_wide = value.astype(jnp.float32)
    blocks = query.reshape(TOKENS // TOK_DEV, TOK_DEV, QH, HD)
    starts = jnp.arange(TOKENS // TOK_DEV, dtype=jnp.int32) * TOK_DEV
    key_pos = jnp.arange(TOKENS, dtype=jnp.int32)

    def one_block(block_inputs):
        block, first = block_inputs
        scores = jnp.einsum('rjd,sd->jrs', block.astype(jnp.float32), key_wide) * scale
        query_pos = first + jnp.arange(TOK_DEV, dtype=jnp.int32)
        allowed = key_pos[None, :] <= query_pos[:, None]
        scores = jnp.where(allowed[None], scores, MASKED)
        top = lax.optimization_barrier(jnp.max(scores, axis=-1, keepdims=True))
        weights = jnp.where(allowed[None], jnp.exp(scores - top), 0.0)
        total = lax.optimization_barrier(jnp.sum(weights, axis=-1))
        result = jnp.einsum('jrs,sd->rjd', weights.astype(jnp.bfloat16).astype(jnp.float32), value_wide)
        return (result / jnp.transpose(total)[:, :, None]).astype(jnp.bfloat16)
    return lax.map(one_block, (blocks, starts)).reshape(TOKENS, QH, HD)

def reference(patches, patch_count, token_patch, window_ids, text_embed, vit_norm_gain, vit_qkv, vit_qkv_bias, vit_proj, vit_proj_bias, merge_norm_gain, merger, merger_bias, llm_norm_gain, w_qkv, qkv_bias):
    normed = rms_norm(patches, vit_norm_gain)
    shard_rows = normed.reshape(N_CTX, TOK_DEV, DV)
    shard_windows = window_ids.reshape(N_CTX, TOK_DEV)

    def one_shard(inputs):
        rows, window_rows, count = inputs
        return vision_heads(rows, vit_qkv, vit_qkv_bias, window_rows, count, VHD)
    attended = lax.map(one_shard, (shard_rows, shard_windows, patch_count)).reshape(TOKENS, DV)
    vit_out = patches.astype(jnp.float32) + jnp.dot(attended, vit_proj, preferred_element_type=jnp.float32) + vit_proj_bias
    merged_in = rms_norm(vit_out, merge_norm_gain)
    image = (jnp.dot(merged_in, merger, preferred_element_type=jnp.float32) + merger_bias).astype(jnp.bfloat16)
    offsets = jnp.arange(TOKENS, dtype=jnp.int32) // TOK_DEV * TOK_DEV
    picked = jnp.take(image, offsets + jnp.maximum(token_patch, 0).astype(jnp.int32), axis=0)
    stitched = jnp.where(token_patch[:, None] >= 0, picked, text_embed)
    values = stitched.astype(jnp.float32)
    llm_in = (values * lax.rsqrt(lax.optimization_barrier(jnp.mean(values * values, axis=-1, keepdims=True)) + EPSILON) * llm_norm_gain).astype(jnp.bfloat16)
    projected = jnp.dot(llm_in, w_qkv, preferred_element_type=jnp.float32) + qkv_bias
    projected = projected.reshape(TOKENS, KVH, QH + 2, HD)
    positions = jnp.arange(TOKENS, dtype=jnp.int32)
    turned = rotate(projected[:, :, :QH + 1], positions).astype(jnp.bfloat16)
    queries = jnp.transpose(turned[:, :, :QH], (1, 0, 2, 3))
    keys_all = jnp.transpose(turned[:, :, QH], (1, 0, 2))
    values_all = jnp.transpose(projected[:, :, QH + 1].astype(jnp.bfloat16), (1, 0, 2))
    context = lax.map(causal_group, (queries, keys_all, values_all))
    return jnp.transpose(context, (1, 0, 2, 3)).reshape(TOKENS, KVH * QH * HD)
```

```python
import math

import jax
import jax.numpy as jnp
from jax import lax
from jax.experimental import pallas as pl
from jax.experimental.pallas import tpu as pltpu
from jax.sharding import PartitionSpec as P

VHD = 80
HD = 128
QH = 4


EPSILON = 1e-06
THETA = 1000000.0
MASKED = -1e30


def rms_norm(rows, gain):
    values = rows.astype(jnp.float32)
    return (
        values * lax.rsqrt(jnp.mean(values * values, axis=-1, keepdims=True) + EPSILON) * gain
    ).astype(jnp.bfloat16)


def rotate(values, positions):
    head_size = values.shape[-1]
    half = head_size // 2
    steps = jnp.arange(half, dtype=jnp.float32) * (2.0 / head_size)
    frequency = jnp.exp(-math.log(THETA) * steps)
    angle = positions.astype(jnp.float32)[:, None] * frequency[None, :]
    cosine = jnp.cos(angle)[:, None, None, :]
    sine = jnp.sin(angle)[:, None, None, :]
    first = values[..., :half]
    second = values[..., half:]
    return jnp.concatenate(
        [first * cosine - second * sine, second * cosine + first * sine], axis=-1
    )


def vision_heads(normed, weight, bias, windows, count, head_size):
    slot_count = normed.shape[0]
    mixed = jnp.dot(normed, weight, preferred_element_type=jnp.float32) + bias
    heads = mixed.shape[1] // (3 * head_size)
    mixed = mixed.astype(jnp.bfloat16).reshape(slot_count, heads, 3, head_size)
    scores = jnp.einsum(
        "rhd,shd->hrs", mixed[:, :, 0], mixed[:, :, 1], preferred_element_type=jnp.float32
    ) * (1.0 / math.sqrt(head_size))
    index = jnp.arange(slot_count, dtype=jnp.int32)
    allowed = (windows[:, None] == windows[None, :]) & (
        (index[None, :] < count) | (index[:, None] == index[None, :])
    )
    scores = jnp.where(allowed[None], scores, MASKED)
    top = jnp.max(scores, axis=-1, keepdims=True)
    weights = jnp.where(allowed[None], jnp.exp(scores - top), 0.0)
    total = jnp.sum(weights, axis=-1)
    result = jnp.einsum(
        "hrs,shd->rhd",
        weights.astype(jnp.bfloat16),
        mixed[:, :, 2],
        preferred_element_type=jnp.float32,
    )
    return (
        (result / jnp.transpose(total)[:, :, None])
        .astype(jnp.bfloat16)
        .reshape(slot_count, heads * head_size)
    )


def attend_block(state, query, query_pos, key, value, key_pos, scale):
    top, total, summed_values = state
    scores = jnp.einsum("gjrd,sgd->gjrs", query, key, preferred_element_type=jnp.float32) * scale
    allowed = key_pos[None, :] <= query_pos[:, None]
    scores = jnp.where(allowed, scores, MASKED)
    new_top = jnp.maximum(top, jnp.max(scores, axis=-1))
    weights = jnp.where(allowed, jnp.exp(scores - new_top[..., None]), 0.0)
    factor = jnp.exp(top - new_top)
    total = total * factor + jnp.sum(weights, axis=-1)
    summed_values = summed_values * factor[..., None] + jnp.einsum(
        "gjrs,sgd->gjrd", weights.astype(jnp.bfloat16), value, preferred_element_type=jnp.float32
    )
    return (new_top, total, summed_values)


def visit_block(state, query, query_pos, key, value, key_pos, scale):
    return lax.cond(
        jnp.min(key_pos) <= jnp.max(query_pos),
        lambda inner: attend_block(inner, query, query_pos, key, value, key_pos, scale),
        lambda inner: inner,
        state,
    )


def general_body(
    patches,
    patch_count,
    token_patch,
    window_ids,
    text_embed,
    vit_norm_gain,
    vit_qkv,
    vit_qkv_bias,
    vit_proj,
    vit_proj_bias,
    merge_norm_gain,
    merger,
    merger_bias,
    llm_norm_gain,
    w_qkv,
    qkv_bias,
):
    ctx_index = lax.axis_index("ctx")
    tok_rows = patches.shape[0]
    half = tok_rows // 2
    normed = rms_norm(patches, vit_norm_gain)
    attended = vision_heads(normed, vit_qkv, vit_qkv_bias, window_ids, patch_count[0], VHD)
    partial_value = jnp.dot(attended, vit_proj, preferred_element_type=jnp.float32)
    summed = lax.psum_scatter(partial_value, "head", scatter_dimension=0, tiled=True)
    share_rows = summed.shape[0]
    own_rows = lax.dynamic_slice_in_dim(patches, lax.axis_index("head") * share_rows, share_rows, 0)
    vit_out = own_rows.astype(jnp.float32) + summed + vit_proj_bias
    merged_share = rms_norm(vit_out, merge_norm_gain)
    merged_in = lax.all_gather(merged_share, "head", axis=0, tiled=True)
    image_sum = jnp.dot(
        merged_in,
        lax.all_gather(merger, "ctx", axis=0, tiled=True),
        preferred_element_type=jnp.float32,
    )
    image = (image_sum + merger_bias).astype(jnp.bfloat16)
    picked = jnp.take(image, jnp.maximum(token_patch, 0), axis=0)
    stitched = jnp.where(token_patch[:, None] >= 0, picked, text_embed)
    whole = lax.all_gather(stitched, "head", axis=1, tiled=True)
    llm_in = rms_norm(whole, llm_norm_gain)
    projected = jnp.dot(
        llm_in, lax.all_gather(w_qkv, "ctx", axis=0, tiled=True), preferred_element_type=jnp.float32
    )
    projected = projected + qkv_bias
    groups = projected.shape[1] // ((QH + 2) * HD)
    projected = projected.reshape(tok_rows, groups, QH + 2, HD)
    positions = ctx_index * tok_rows + jnp.arange(tok_rows, dtype=jnp.int32)
    turned = rotate(projected[:, :, : QH + 1], positions).astype(jnp.bfloat16)
    queries = turned[:, :, :QH].reshape(tok_rows, groups * QH * HD)
    key_rows = turned[:, :, QH].reshape(tok_rows, groups * HD)
    value_rows = projected[:, :, QH + 1].astype(jnp.bfloat16).reshape(tok_rows, groups * HD)
    first_pos = ctx_index * tok_rows + jnp.arange(half, dtype=jnp.int32)
    second_pos = first_pos + half
    scale = 1.0 / math.sqrt(HD)
    query_heads = jnp.transpose(queries.reshape(tok_rows, groups, QH, HD), (1, 2, 0, 3))
    blocks = (query_heads[:, :, :half], query_heads[:, :, half:])
    block_pos = (first_pos, second_pos)

    def fresh():
        return (
            jnp.full((groups, QH, half), MASKED, jnp.float32),
            jnp.zeros((groups, QH, half), jnp.float32),
            jnp.zeros((groups, QH, half, HD), jnp.float32),
        )

    key_piece = lax.all_gather(key_rows, "ctx", axis=0, tiled=True)
    value_piece = lax.all_gather(value_rows, "ctx", axis=0, tiled=True)
    piece_rows = key_piece.shape[0]
    block_rows = math.gcd(piece_rows, tok_rows)
    block_count = piece_rows // block_rows
    key_piece = key_piece.reshape(block_count, block_rows, groups, HD)
    value_piece = value_piece.reshape(block_count, block_rows, groups, HD)

    def visit(index, states):
        key_block = lax.dynamic_index_in_dim(key_piece, index, 0, keepdims=False)
        value_block = lax.dynamic_index_in_dim(value_piece, index, 0, keepdims=False)
        row_index = index * block_rows + jnp.arange(block_rows, dtype=jnp.int32)
        updated = []
        for which in range(2):
            updated.append(
                visit_block(
                    states[which],
                    blocks[which],
                    block_pos[which],
                    key_block,
                    value_block,
                    row_index,
                    scale,
                )
            )
        return tuple(updated)

    carry = lax.fori_loop(0, block_count, visit, (fresh(), fresh()))
    outputs = []
    for state in carry:
        top, total, summed_values = state
        result = (summed_values / total[..., None]).astype(jnp.bfloat16)
        outputs.append(jnp.transpose(result, (2, 0, 1, 3)).reshape(half, groups * QH * HD))
    return jnp.concatenate(outputs, axis=0)


def any_spec():
    return pl.BlockSpec(memory_space=pl.ANY)


def vmem_spec():
    return pl.BlockSpec(memory_space=pltpu.VMEM)


def smem_spec():
    return pl.BlockSpec(memory_space=pltpu.SMEM)


def image_kernel(blocks, merged_ref, text_ref, slot_ref, bias_ref, blk_ref, *rest):
    pieces = rest[:blocks]
    out_ref, weight, sems = rest[blocks:]
    rows = pieces[0].shape[0]
    copies = []
    for k in range(blocks):
        copies.append(
            pltpu.make_async_copy(
                pieces[k], weight.at[pl.ds(blk_ref[k] * rows, rows), :], sems.at[k]
            )
        )
    for copy in copies:
        copy.start()
    slots = slot_ref[...]
    count = slots.shape[0]
    chosen = (lax.broadcasted_iota(jnp.int32, (count, count), 1) == slots).astype(jnp.bfloat16)
    for copy in copies:
        copy.wait()
    image = jnp.dot(merged_ref[...], weight[...], preferred_element_type=jnp.float32)
    image = (image + bias_ref[...]).astype(jnp.bfloat16)
    picked = jnp.dot(chosen, image, preferred_element_type=jnp.float32).astype(jnp.bfloat16)
    out_ref[...] = jnp.where(slots >= 0, picked, text_ref[...])


def turn(x, cosine, sine):
    return x * cosine + pltpu.roll(x, x.shape[1] // 2, 1) * sine


def key_kernel(
    lines, blocks, own_cols, gain_ref, bias_ref, cos_ref, sin_ref, blk_ref, *rest
):
    halves = (rest[:lines], rest[lines : 2 * lines])
    pieces = rest[2 * lines : 2 * lines + blocks]
    kv_ref, llm_ref, weight, sems = rest[2 * lines + blocks :]
    rows = pieces[0].shape[0]
    width = weight.shape[1]
    start = pieces[0].shape[1] - width
    copies = []
    for k in range(blocks):
        copies.append(
            pltpu.make_async_copy(
                pieces[k].at[:, pl.ds(start, width)],
                weight.at[pl.ds(blk_ref[k] * rows, rows), :],
                sems.at[k],
            )
        )
    for copy in copies:
        copy.start()
    for s in range(lines):
        first = halves[0][s][...].astype(jnp.float32)
        second = halves[1][s][...].astype(jnp.float32)
        total = jnp.sum(first * first, axis=-1, keepdims=True) + jnp.sum(
            second * second, axis=-1, keepdims=True
        )
        factor = lax.rsqrt(total / (2.0 * own_cols) + EPSILON)
        llm_ref[s, :, :own_cols] = (first * factor * gain_ref[:, :own_cols]).astype(jnp.bfloat16)
        llm_ref[s, :, own_cols:] = (second * factor * gain_ref[:, own_cols:]).astype(jnp.bfloat16)
    for copy in copies:
        copy.wait()
    for s in range(lines):
        projected = jnp.dot(llm_ref[s], weight[...], preferred_element_type=jnp.float32)
        projected = projected + bias_ref[...]
        kv_ref[s, :, :HD] = turn(projected[:, :HD], cos_ref[s], sin_ref[s]).astype(jnp.bfloat16)
        kv_ref[s, :, HD:] = projected[:, HD:].astype(jnp.bfloat16)


def query_kernel(lines, blocks, llm_ref, bias_ref, cos_ref, sin_ref, blk_ref, *rest):
    pieces = rest[:blocks]
    q_ref, weight, sems = rest[blocks:]
    rows = pieces[0].shape[0]
    width = weight.shape[1]
    copies = []
    for k in range(blocks):
        copies.append(
            pltpu.make_async_copy(
                pieces[k].at[:, pl.ds(0, width)],
                weight.at[pl.ds(blk_ref[k] * rows, rows), :],
                sems.at[k],
            )
        )
    for copy in copies:
        copy.start()
    for copy in copies:
        copy.wait()
    tokens = llm_ref.shape[1]
    for s in range(lines):
        projected = jnp.dot(llm_ref[s], weight[...], preferred_element_type=jnp.float32)
        projected = projected + bias_ref[...]
        for j in range(QH):
            head = turn(projected[:, j * HD : (j + 1) * HD], cos_ref[s], sin_ref[s])
            q_ref[s, j * tokens : (j + 1) * tokens, :] = head.astype(jnp.bfloat16)


def attend_kernel(lines, lanes, tokens, place_ref, blk_ref, q_ref, *rest):
    pieces = rest[:lanes]
    o_ref, kv, sems = rest[lanes:]
    copies = []
    for d in range(lanes):
        for s in range(lines):
            copies.append(
                pltpu.make_async_copy(
                    pieces[d].at[s],
                    kv.at[pl.ds(blk_ref[s * lanes + d] * tokens, tokens), :],
                    sems.at[s * lanes + d],
                )
            )
    for copy in copies:
        copy.start()
    for copy in copies:
        copy.wait()
    lane = place_ref[lines]
    span = lanes * tokens
    scale = 1.0 / math.sqrt(HD)
    rows = QH * tokens
    row_pos = lane * tokens + lax.rem(lax.broadcasted_iota(jnp.int32, (rows, span), 0), tokens)
    visible = lax.broadcasted_iota(jnp.int32, (rows, span), 1) <= row_pos

    def one_line(s, unused):
        query = q_ref[s]

        def visit(chunk, state, masked):
            top, total, summed = state
            at = pl.multiple_of(chunk * span, span)
            key = kv[pl.ds(at, span), :HD]
            value = kv[pl.ds(at, span), HD:]
            scores = (
                lax.dot_general(
                    query, key, (((1,), (1,)), ((), ())), preferred_element_type=jnp.float32
                )
                * scale
            )
            if masked:
                scores = jnp.where(visible, scores, MASKED)
            new_top = jnp.maximum(top, jnp.max(scores, axis=-1, keepdims=True))
            weights = jnp.exp(scores - new_top)
            factor = jnp.exp(top - new_top)
            total = total * factor + jnp.sum(weights, axis=-1, keepdims=True)
            summed = summed * factor + jnp.dot(
                weights.astype(jnp.bfloat16), value, preferred_element_type=jnp.float32
            )
            return new_top, total, summed

        line = place_ref[s]
        state = (
            jnp.full((rows, 1), MASKED, jnp.float32),
            jnp.zeros((rows, 1), jnp.float32),
            jnp.zeros((rows, HD), jnp.float32),
        )
        state = visit(line, state, True)
        state = lax.fori_loop(0, line, lambda c, st: visit(c, st, False), state)
        top, total, summed = state
        result = (summed / total).astype(jnp.bfloat16)
        for j in range(QH):
            o_ref[s, :, j * HD : (j + 1) * HD] = result[j * tokens : (j + 1) * tokens, :]
        return unused

    lax.fori_loop(0, lines, one_line, 0)


def place_kernel(lines, place_ref, *rest):
    pieces = rest[:lines]
    o_ref, sems = rest[lines:]
    width = pieces[0].shape[1]
    copies = []
    for s in range(lines):
        copies.append(
            pltpu.make_async_copy(
                pieces[s], o_ref.at[:, pl.ds(place_ref[s] * width, width)], sems.at[s]
            )
        )
    for copy in copies:
        copy.start()
    for copy in copies:
        copy.wait()


def plane_body(lines, lanes):
    size = lines * lanes

    def hop(x, mask):
        return lax.ppermute(x, "ctx", [(c, c ^ mask) for c in range(size)])

    def swap(x):
        return lax.ppermute(x, "head", [(0, 1), (1, 0)])

    def plane_gather(pieces):
        one = [hop(p, 1) for p in pieces]
        two = [hop(p, 2) for p in pieces]
        three = []
        for s in range(len(pieces)):
            three.append(hop(one[s], 2) if s % 2 == 0 else hop(two[s], 1))
        return (pieces, one, two, three)

    def body(
        patches,
        patch_count,
        token_patch,
        window_ids,
        text_embed,
        vit_norm_gain,
        vit_qkv,
        vit_qkv_bias,
        vit_proj,
        vit_proj_bias,
        merge_norm_gain,
        merger,
        merger_bias,
        llm_norm_gain,
        w_qkv,
        qkv_bias,
    ):
        ctx_index = lax.axis_index("ctx")
        line = ctx_index // lanes
        lane = ctx_index % lanes
        side = lax.axis_index("head")
        tokens = patches.shape[0]
        own_cols = text_embed.shape[1]
        group_cols = (QH + 2) * HD
        line_of = [line ^ s for s in range(lines)]
        blocks = size

        merger_line = [merger] + [hop(merger, s * lanes) for s in range(1, lines)]
        merger_all = plane_gather(merger_line)
        columns = [
            lax.dynamic_slice_in_dim(w_qkv, line_of[s] * group_cols, group_cols, 1)
            for s in range(lines)
        ]
        weight_line = [columns[0]] + [hop(columns[s], s * lanes) for s in range(1, lines)]
        weight_all = plane_gather(weight_line)

        order = [(s, d) for s in range(lines) for d in range(lanes)]
        block_of = jnp.stack([line_of[s] * lanes + (lane ^ d) for s, d in order]).astype(jnp.int32)
        turned_block = block_of ^ (side * (blocks // 2))
        places = jnp.stack(line_of + [lane]).astype(jnp.int32)

        normed = rms_norm(patches, vit_norm_gain)
        attended = vision_heads(normed, vit_qkv, vit_qkv_bias, window_ids, patch_count[0], VHD)
        part = jnp.dot(attended, vit_proj, preferred_element_type=jnp.float32)
        vit_out = patches.astype(jnp.float32) + (part + swap(part)) + vit_proj_bias
        merged_in = rms_norm(vit_out, merge_norm_gain)

        stitched = pl.pallas_call(
            lambda *refs: image_kernel(blocks, *refs),
            out_shape=jax.ShapeDtypeStruct(text_embed.shape, jnp.bfloat16),
            in_specs=[vmem_spec()] * 4 + [smem_spec()] + [any_spec()] * blocks,
            out_specs=vmem_spec(),
            scratch_shapes=[
                pltpu.VMEM((merger.shape[0] * size, merger.shape[1]), jnp.bfloat16),
                pltpu.SemaphoreType.DMA((blocks,)),
            ],
            name="image",
        )(
            merged_in,
            text_embed,
            token_patch.reshape(tokens, 1),
            merger_bias.reshape(1, -1),
            block_of,
            *[merger_all[d][s] for s, d in order],
        )

        own_half = [stitched] + [hop(stitched, s * lanes) for s in range(1, lines)]
        other_half = [swap(x) for x in own_half]

        half = HD // 2
        steps = jnp.arange(half, dtype=jnp.float32) * (2.0 / HD)
        frequency = jnp.exp(-math.log(THETA) * steps)
        positions = jnp.stack(
            [
                (line_of[s] * lanes + lane) * tokens + jnp.arange(tokens, dtype=jnp.int32)
                for s in range(lines)
            ]
        )
        angle = positions.astype(jnp.float32)[..., None] * frequency
        cosine = jnp.cos(angle)
        sine = jnp.sin(angle)
        cosine = jnp.concatenate([cosine, cosine], axis=-1)
        sine = jnp.concatenate([-sine, sine], axis=-1)

        gain = lax.dynamic_slice_in_dim(
            jnp.concatenate([llm_norm_gain, llm_norm_gain[:own_cols]]),
            side * own_cols,
            2 * own_cols,
            0,
        ).reshape(1, -1)
        bias = lax.dynamic_slice_in_dim(qkv_bias, line * group_cols, group_cols, 0).reshape(1, -1)
        weight_list = [weight_all[d][s] for s, d in order]
        depth = w_qkv.shape[0] * size

        kv, llm_in = pl.pallas_call(
            lambda *refs: key_kernel(lines, blocks, own_cols, *refs),
            out_shape=(
                jax.ShapeDtypeStruct((lines, tokens, 2 * HD), jnp.bfloat16),
                jax.ShapeDtypeStruct((lines, tokens, 2 * own_cols), jnp.bfloat16),
            ),
            in_specs=[vmem_spec()] * 4
            + [smem_spec()]
            + [vmem_spec()] * (2 * lines)
            + [any_spec()] * blocks,
            out_specs=(vmem_spec(), vmem_spec()),
            scratch_shapes=[
                pltpu.VMEM((depth, 2 * HD), jnp.bfloat16),
                pltpu.SemaphoreType.DMA((blocks,)),
            ],
            name="keys",
        )(
            gain,
            bias[:, QH * HD :],
            cosine,
            sine,
            turned_block,
            *own_half,
            *other_half,
            *weight_list,
        )

        kv_all = [kv, hop(kv, 1), hop(kv, 2), hop(kv, 3)]

        query = pl.pallas_call(
            lambda *refs: query_kernel(lines, blocks, *refs),
            out_shape=jax.ShapeDtypeStruct((lines, QH * tokens, HD), jnp.bfloat16),
            in_specs=[vmem_spec()] * 4 + [smem_spec()] + [any_spec()] * blocks,
            out_specs=vmem_spec(),
            scratch_shapes=[
                pltpu.VMEM((depth, QH * HD), jnp.bfloat16),
                pltpu.SemaphoreType.DMA((blocks,)),
            ],
            name="queries",
        )(llm_in, bias[:, : QH * HD], cosine, sine, turned_block, *weight_list)

        context = pl.pallas_call(
            lambda *refs: attend_kernel(lines, lanes, tokens, *refs),
            out_shape=jax.ShapeDtypeStruct((lines, tokens, QH * HD), jnp.bfloat16),
            in_specs=[smem_spec(), smem_spec(), vmem_spec()] + [any_spec()] * lanes,
            out_specs=vmem_spec(),
            scratch_shapes=[
                pltpu.VMEM((size * tokens, 2 * HD), jnp.bfloat16),
                pltpu.SemaphoreType.DMA((blocks,)),
            ],
            name="attend",
        )(places, block_of, query, *kv_all)

        returned = [context[0]] + [hop(context[s], s * lanes) for s in range(1, lines)]
        return pl.pallas_call(
            lambda *refs: place_kernel(lines, *refs),
            out_shape=jax.ShapeDtypeStruct((tokens, lines * QH * HD), jnp.bfloat16),
            in_specs=[smem_spec()] + [any_spec()] * lines,
            out_specs=any_spec(),
            scratch_shapes=[pltpu.SemaphoreType.DMA((lines,))],
            name="place",
        )(places, *returned)

    return body


def plane_shape(mesh):
    def pick(w_shape):
        groups = w_shape[1] // mesh.shape["head"] // ((QH + 2) * HD)
        size = mesh.shape["ctx"]
        if mesh.shape["head"] == 2 and groups == 4 and size == groups * groups:
            return groups, size // groups
        return None

    return pick


def solution(mesh):
    specs = (
        P("ctx", None),
        P("ctx"),
        P("ctx"),
        P("ctx"),
        P("ctx", "head"),
        P(),
        P(None, "head"),
        P("head"),
        P("head", None),
        P(),
        P(),
        P("ctx", "head"),
        P("head"),
        P(),
        P("ctx", "head"),
        P("head"),
    )

    def run(*arrays):
        shape = plane_shape(mesh)(arrays[14].shape)
        body = general_body if shape is None else plane_body(*shape)
        return jax.shard_map(
            body, mesh=mesh, in_specs=specs, out_specs=P("ctx", "head"), check_vma=False
        )(*arrays)

    return run
```

```python
import math

import jax
import jax.numpy as jnp
from jax import lax
from jax.experimental import pallas as pl
from jax.experimental.pallas import tpu as pltpu
from jax.sharding import PartitionSpec as P


VHD = 80
HD = 128
QH = 4
KVH = 8


EPSILON = 1e-06
THETA = 1000000.0
MASKED = -1e30


def rms_norm(rows, gain):
    values = rows.astype(jnp.float32)
    return (
        values * lax.rsqrt(jnp.mean(values * values, axis=-1, keepdims=True) + EPSILON) * gain
    ).astype(jnp.bfloat16)


def rotate(values, positions):
    head_size = values.shape[-1]
    half = head_size // 2
    steps = jnp.arange(half, dtype=jnp.float32) * (2.0 / head_size)
    frequency = jnp.exp(-math.log(THETA) * steps)
    angle = positions.astype(jnp.float32)[:, None] * frequency[None, :]
    cosine = jnp.cos(angle)[:, None, None, :]
    sine = jnp.sin(angle)[:, None, None, :]
    first = values[..., :half]
    second = values[..., half:]
    return jnp.concatenate(
        [first * cosine - second * sine, second * cosine + first * sine], axis=-1
    )


def vision_heads(normed, weight, bias, windows, count, head_size):
    slot_count = normed.shape[0]
    heads = weight.shape[1] // (3 * head_size)
    mixed = jnp.dot(normed, weight, preferred_element_type=jnp.float32) + bias
    mixed = mixed.astype(jnp.bfloat16).reshape(slot_count, heads, 3, head_size)
    return vision_weights(mixed, windows, count)


def vision_weights(mixed, windows, count):
    slot_count, heads, _, head_size = mixed.shape
    scores = jnp.einsum(
        "rhd,shd->hrs", mixed[:, :, 0], mixed[:, :, 1], preferred_element_type=jnp.float32
    ) * (1.0 / math.sqrt(head_size))
    index = jnp.arange(slot_count, dtype=jnp.int32)
    allowed = (windows[:, None] == windows[None, :]) & (
        (index[None, :] < count) | (index[:, None] == index[None, :])
    )
    scores = jnp.where(allowed[None], scores, MASKED)
    top = jnp.max(scores, axis=-1, keepdims=True)
    weights = jnp.where(allowed[None], jnp.exp(scores - top), 0.0)
    total = jnp.sum(weights, axis=-1)
    result = jnp.einsum(
        "hrs,shd->rhd",
        weights.astype(jnp.bfloat16),
        mixed[:, :, 2],
        preferred_element_type=jnp.float32,
    )
    return (
        (result / jnp.transpose(total)[:, :, None])
        .astype(jnp.bfloat16)
        .reshape(slot_count, heads * head_size)
    )


def attend_block(state, query, query_pos, key, value, key_pos, scale):
    top, total, summed_values = state
    scores = jnp.einsum("gjrd,sgd->gjrs", query, key, preferred_element_type=jnp.float32) * scale
    allowed = key_pos[None, :] <= query_pos[:, None]
    scores = jnp.where(allowed, scores, MASKED)
    new_top = jnp.maximum(top, jnp.max(scores, axis=-1))
    weights = jnp.where(allowed, jnp.exp(scores - new_top[..., None]), 0.0)
    factor = jnp.exp(top - new_top)
    total = total * factor + jnp.sum(weights, axis=-1)
    summed_values = summed_values * factor[..., None] + jnp.einsum(
        "gjrs,sgd->gjrd", weights.astype(jnp.bfloat16), value, preferred_element_type=jnp.float32
    )
    return (new_top, total, summed_values)


def visit_block(state, query, query_pos, key, value, key_pos, scale):
    return lax.cond(
        jnp.min(key_pos) <= jnp.max(query_pos),
        lambda inner: attend_block(inner, query, query_pos, key, value, key_pos, scale),
        lambda inner: inner,
        state,
    )


def general_body(
    patches,
    patch_count,
    token_patch,
    window_ids,
    text_embed,
    vit_norm_gain,
    vit_qkv,
    vit_qkv_bias,
    vit_proj,
    vit_proj_bias,
    merge_norm_gain,
    merger,
    merger_bias,
    llm_norm_gain,
    w_qkv,
    qkv_bias,
):
    ctx_index = lax.axis_index("ctx")
    tok_rows = patches.shape[0]
    half = tok_rows // 2
    normed = rms_norm(patches, vit_norm_gain)
    attended = vision_heads(normed, vit_qkv, vit_qkv_bias, window_ids, patch_count[0], VHD)
    partial_value = jnp.dot(attended, vit_proj, preferred_element_type=jnp.float32)
    summed = lax.psum_scatter(partial_value, "head", scatter_dimension=0, tiled=True)
    share_rows = summed.shape[0]
    own_rows = lax.dynamic_slice_in_dim(patches, lax.axis_index("head") * share_rows, share_rows, 0)
    vit_out = own_rows.astype(jnp.float32) + summed + vit_proj_bias
    merged_share = rms_norm(vit_out, merge_norm_gain)
    merged_in = lax.all_gather(merged_share, "head", axis=0, tiled=True)
    image_sum = jnp.dot(
        merged_in,
        lax.all_gather(merger, "ctx", axis=0, tiled=True),
        preferred_element_type=jnp.float32,
    )
    image = (image_sum + merger_bias).astype(jnp.bfloat16)
    picked = jnp.take(image, jnp.maximum(token_patch, 0), axis=0)
    stitched = jnp.where(token_patch[:, None] >= 0, picked, text_embed)
    whole = lax.all_gather(stitched, "head", axis=1, tiled=True)
    llm_in = rms_norm(whole, llm_norm_gain)
    projected = jnp.dot(
        llm_in, lax.all_gather(w_qkv, "ctx", axis=0, tiled=True), preferred_element_type=jnp.float32
    )
    projected = projected + qkv_bias
    groups = projected.shape[1] // ((QH + 2) * HD)
    projected = projected.reshape(tok_rows, groups, QH + 2, HD)
    positions = ctx_index * tok_rows + jnp.arange(tok_rows, dtype=jnp.int32)
    turned = rotate(projected[:, :, : QH + 1], positions).astype(jnp.bfloat16)
    queries = turned[:, :, :QH].reshape(tok_rows, groups * QH * HD)
    key_rows = turned[:, :, QH].reshape(tok_rows, groups * HD)
    value_rows = projected[:, :, QH + 1].astype(jnp.bfloat16).reshape(tok_rows, groups * HD)
    first_pos = ctx_index * tok_rows + jnp.arange(half, dtype=jnp.int32)
    second_pos = first_pos + half
    scale = 1.0 / math.sqrt(HD)
    query_heads = jnp.transpose(queries.reshape(tok_rows, groups, QH, HD), (1, 2, 0, 3))
    blocks = (query_heads[:, :, :half], query_heads[:, :, half:])
    block_pos = (first_pos, second_pos)

    def fresh():
        return (
            jnp.full((groups, QH, half), MASKED, jnp.float32),
            jnp.zeros((groups, QH, half), jnp.float32),
            jnp.zeros((groups, QH, half, HD), jnp.float32),
        )

    key_piece = lax.all_gather(key_rows, "ctx", axis=0, tiled=True)
    value_piece = lax.all_gather(value_rows, "ctx", axis=0, tiled=True)
    piece_rows = key_piece.shape[0]
    block_rows = math.gcd(piece_rows, tok_rows)
    block_count = piece_rows // block_rows
    key_piece = key_piece.reshape(block_count, block_rows, groups, HD)
    value_piece = value_piece.reshape(block_count, block_rows, groups, HD)

    def visit(index, states):
        key_block = lax.dynamic_index_in_dim(key_piece, index, 0, keepdims=False)
        value_block = lax.dynamic_index_in_dim(value_piece, index, 0, keepdims=False)
        row_index = index * block_rows + jnp.arange(block_rows, dtype=jnp.int32)
        updated = []
        for which in range(2):
            updated.append(
                visit_block(
                    states[which],
                    blocks[which],
                    block_pos[which],
                    key_block,
                    value_block,
                    row_index,
                    scale,
                )
            )
        return tuple(updated)

    carry = lax.fori_loop(0, block_count, visit, (fresh(), fresh()))
    outputs = []
    for state in carry:
        _, total, summed_values = state
        result = (summed_values / total[..., None]).astype(jnp.bfloat16)
        outputs.append(jnp.transpose(result, (2, 0, 1, 3)).reshape(half, groups * QH * HD))
    return jnp.concatenate(outputs, axis=0)


def any_spec():
    return pl.BlockSpec(memory_space=pl.ANY)


def vmem_spec():
    return pl.BlockSpec(memory_space=pltpu.VMEM)


def smem_spec():
    return pl.BlockSpec(memory_space=pltpu.SMEM)


def image_kernel(lines, lanes, place_ref, merged_ref, near_ref, far_ref, *rest):
    packed = rest[:lines]
    pieces = rest[lines : lines + lanes]
    out_ref, left, weight = rest[lines + lanes :]
    line = place_ref[0]
    lane = place_ref[1]
    side = place_ref[2]
    mine = place_ref[3]
    tokens = merged_ref.shape[0]
    share = tokens // 2
    rows = pieces[0].shape[0] // lines
    left[pl.ds(pl.multiple_of(line * tokens, tokens), tokens), :] = merged_ref[...]
    for s in range(1, lines):
        base = (line ^ s) * tokens
        near = pl.multiple_of(base + side * share, share)
        far = pl.multiple_of(base + (1 - side) * share, share)
        left[pl.ds(near, share), :] = near_ref[(s - 1) * share : s * share, :]
        left[pl.ds(far, share), :] = far_ref[(s - 1) * share : s * share, :]
    for d in range(lanes):
        for r in range(lines):
            block = (mine ^ r) * lanes + (lane ^ d)
            at = pl.multiple_of(block * rows, 16)
            weight[pl.ds(at, rows), :] = pieces[d][r * rows : (r + 1) * rows, :]
    extra = packed[0][tokens + rows : tokens + rows + 16, :].astype(jnp.float32)
    bias = extra[1:2, :] + extra[2:3, :] + extra[3:4, :]
    patch = lax.broadcasted_iota(jnp.int32, (tokens, tokens), 0).astype(jnp.float32)
    ones = jnp.ones((tokens, tokens), jnp.bfloat16)
    sublane = (((0,), (0,)), ((), ()))
    image = jnp.dot(left[...], weight[...], preferred_element_type=jnp.float32)
    left_image = (image + bias).astype(jnp.bfloat16)
    out_ref[...] = left_image
    for r in range(lines):
        at = pl.multiple_of((mine ^ r) * tokens, tokens)
        rows_image = out_ref[pl.ds(at, tokens), :]
        slots = packed[r][tokens + rows : tokens + rows + 16, :tokens].astype(jnp.float32)
        chosen = (patch == slots[:1, :]).astype(jnp.float32).astype(jnp.bfloat16)
        picked = lax.dot_general(chosen, rows_image, sublane, preferred_element_type=jnp.float32)
        found = lax.dot_general(chosen, ones, sublane, preferred_element_type=jnp.float32)
        out_ref[pl.ds(at, tokens), :] = jnp.where(
            found[:, :1] > 0.5, picked.astype(jnp.bfloat16), packed[r][:tokens, :]
        )


def cut_kernel(width, place_ref, w_ref, *outs):
    for s, o_ref in zip((2, 0, 3, 1), outs):
        at = pl.multiple_of((place_ref[0] ^ s) * width, width)
        o_ref[...] = w_ref[:, pl.ds(at, width)]


def pack_kernel(place_ref, text_ref, merger_ref, slot_ref, bias_ref, *outs):
    tokens = text_ref.shape[0]
    rows = merger_ref.shape[0]
    width = outs[0].shape[1]
    row = lax.broadcasted_iota(jnp.int32, (16, width), 0)
    slots = jnp.concatenate(
        [slot_ref[...].astype(jnp.float32), jnp.zeros((1, width - tokens), jnp.float32)], axis=1
    )
    for r, o_ref in enumerate(outs):
        cols = pl.ds(pl.multiple_of((place_ref[0] ^ r) * width, width), width)
        o_ref[:tokens, :] = text_ref[:, cols]
        o_ref[tokens : tokens + rows, :] = merger_ref[:, cols]
        bias = bias_ref[:, cols]
        high = bias.astype(jnp.bfloat16).astype(jnp.float32)
        middle = (bias - high).astype(jnp.bfloat16).astype(jnp.float32)
        low = bias - high - middle
        extra = jnp.where(row == 0, slots, 0.0)
        for at, value in ((1, high), (2, middle), (3, low)):
            extra = jnp.where(row == at, value, extra)
        o_ref[tokens + rows :, :] = extra.astype(jnp.bfloat16)


def collect_kernel(lanes, place_ref, *rest):
    pieces = rest[: 2 * lanes]
    w_ref, sems = rest[2 * lanes :]
    rows = pieces[0].shape[0]
    copies = []
    for e in range(2):
        for d in range(lanes):
            block = ((place_ref[0] % 2) ^ e) * lanes + (place_ref[1] ^ d)
            copies.append(
                pltpu.make_async_copy(
                    pieces[e * lanes + d],
                    w_ref.at[pl.ds(block * rows, rows), :],
                    sems.at[e * lanes + d],
                )
            )
    for copy in copies:
        copy.start()
    for copy in copies:
        copy.wait()


def add_blocks(blocks, pieces, cols, place_ref, gain_ref, w_ref, total):
    squares = None
    for e, piece in zip(blocks, pieces):
        width = piece.shape[1]
        at = pl.multiple_of((place_ref[3] ^ e) * width, width)
        depth = w_ref.shape[0]
        gain_at = pl.multiple_of((place_ref[0] // 2) * depth + at, width)
        rows = piece[...].astype(jnp.float32)
        more = jnp.sum(rows * rows, axis=-1, keepdims=True)
        squares = more if squares is None else squares + more
        scaled = (rows * gain_ref[:, pl.ds(gain_at, width)]).astype(jnp.bfloat16)
        product = jnp.dot(
            scaled, w_ref[pl.ds(at, width), cols], preferred_element_type=jnp.float32
        )
        total = product if total is None else total + product
    return total, squares


def partial_kernel(blocks, place_ref, gain_ref, w_ref, *rest):
    pieces = rest[: len(blocks)]
    sum_ref, square_ref = rest[len(blocks) :]
    total, squares = add_blocks(
        blocks, pieces, slice(0, w_ref.shape[1]), place_ref, gain_ref, w_ref, None
    )
    sum_ref[...] = total
    square_ref[...] = jnp.broadcast_to(squares, square_ref.shape)


def send_keys_kernel(blocks, place_ref, gain_ref, w_ref, *rest):
    pieces = rest[: len(blocks)]
    sum_ref, square_ref, out_ref, all_ref, row_ref = rest[len(blocks) :]
    cols = slice(QH * HD, w_ref.shape[1])
    total, squares = add_blocks(
        blocks, pieces, cols, place_ref, gain_ref, w_ref, sum_ref[:, cols]
    )
    out_ref[...] = total.astype(jnp.bfloat16)
    squares = square_ref[...] + jnp.broadcast_to(squares, square_ref.shape)
    all_ref[...] = squares
    row_ref[...] = jnp.transpose(squares)[: row_ref.shape[0], :]


def send_queries_kernel(blocks, place_ref, gain_ref, w_ref, *rest):
    pieces = rest[: len(blocks)]
    sum_ref, out_ref = rest[len(blocks) :]
    cols = slice(0, QH * HD)
    total, _ = add_blocks(blocks, pieces, cols, place_ref, gain_ref, w_ref, sum_ref[:, cols])
    out_ref[...] = total.astype(jnp.bfloat16)


def keep_kernel(blocks, place_ref, gain_ref, w_ref, *rest):
    pieces = rest[: len(blocks)]
    out_ref = rest[len(blocks)]
    cols = slice(0, w_ref.shape[1])
    out_ref[...] = add_blocks(blocks, pieces, cols, place_ref, gain_ref, w_ref, None)[0]


def row_factor(depth, all_ref, row_ref):
    rows = jnp.broadcast_to(row_ref[:1, :], (all_ref.shape[1], row_ref.shape[1]))
    squares = all_ref[...] + jnp.transpose(rows)
    return lax.rsqrt(squares / depth + EPSILON)


def turn(x, cosine, sine):
    return x * cosine + pltpu.roll(x, x.shape[1] // 2, 1) * sine


def key_kernel(depth, bias_ref, cos_ref, sin_ref, place_ref, all_ref, row_ref, *rest):
    keep_ref, got_ref, kv_ref = rest
    factor = row_factor(depth, all_ref, row_ref)
    group = keep_ref.shape[1]
    at = pl.multiple_of(place_ref[0] * group + QH * HD, HD)
    total = keep_ref[:, QH * HD :] + got_ref[...].astype(jnp.float32)
    key = total[:, :HD] * factor + bias_ref[:, pl.ds(at, HD)]
    value = total[:, HD:] * factor + bias_ref[:, pl.ds(at + HD, HD)]
    kv_ref[:, :HD] = turn(key, cos_ref[...], sin_ref[...]).astype(jnp.bfloat16)
    kv_ref[:, HD:] = value.astype(jnp.bfloat16)


def query_kernel(depth, bias_ref, cos_ref, sin_ref, place_ref, all_ref, row_ref, *rest):
    keep_ref, got_ref, q_ref = rest
    factor = row_factor(depth, all_ref, row_ref)
    lines = q_ref.shape[0]
    tokens = keep_ref.shape[0] // lines
    group = keep_ref.shape[1]
    for j in range(QH):
        cols = slice(j * HD, (j + 1) * HD)
        at = pl.multiple_of(place_ref[0] * group + j * HD, HD)
        total = keep_ref[:, cols] + got_ref[:, cols].astype(jnp.float32)
        head = turn(total * factor + bias_ref[:, pl.ds(at, HD)], cos_ref[...], sin_ref[...])
        head = head.astype(jnp.bfloat16)
        for s in range(lines):
            q_ref[s, j * tokens : (j + 1) * tokens, :] = head[s * tokens : (s + 1) * tokens, :]


def gather_kernel(lines, lanes, place_ref, *rest):
    pieces = rest[:lanes]
    kv_ref = rest[lanes]
    tokens = kv_ref.shape[0] // (lines * lanes)
    for d in range(lanes):
        for z in range(lines):
            at = pl.multiple_of((z * lanes + (place_ref[1] ^ d)) * tokens, tokens)
            kv_ref[pl.ds(at, tokens), :] = pieces[d][z * tokens : (z + 1) * tokens, :]


def attend_kernel(which, lanes, place_ref, kv, q_ref, *outs):
    tokens = outs[0].shape[0]
    lane = place_ref[1]
    span = lanes * tokens
    scale = 1.0 / math.sqrt(HD)
    rows = QH * tokens
    row_pos = lane * tokens + lax.rem(lax.broadcasted_iota(jnp.int32, (rows, span), 0), tokens)
    visible = lax.broadcasted_iota(jnp.int32, (rows, span), 1) <= row_pos

    for o_ref, s in zip(outs, which):
        query = q_ref[place_ref[0] ^ s]

        def visit(chunk, state, masked):
            top, total, summed = state
            at = pl.multiple_of(chunk * span, span)
            key = kv[pl.ds(at, span), :HD]
            value = kv[pl.ds(at, span), HD:]
            scores = (
                lax.dot_general(
                    query, key, (((1,), (1,)), ((), ())), preferred_element_type=jnp.float32
                )
                * scale
            )
            if masked:
                scores = jnp.where(visible, scores, MASKED)
            new_top = jnp.maximum(top, jnp.max(scores, axis=-1, keepdims=True))
            weights = jnp.exp(scores - new_top)
            factor = jnp.exp(top - new_top)
            total = total * factor + jnp.sum(weights, axis=-1, keepdims=True)
            summed = summed * factor + jnp.dot(
                weights.astype(jnp.bfloat16), value, preferred_element_type=jnp.float32
            )
            return new_top, total, summed

        line = place_ref[0] ^ s
        state = (
            jnp.full((rows, 1), MASKED, jnp.float32),
            jnp.zeros((rows, 1), jnp.float32),
            jnp.zeros((rows, HD), jnp.float32),
        )
        state = visit(line, state, True)
        state = lax.fori_loop(0, line, lambda c, st: visit(c, st, False), state)
        _, total, summed = state
        result = (summed / total).astype(jnp.bfloat16)
        for j in range(QH):
            o_ref[:, j * HD : (j + 1) * HD] = result[j * tokens : (j + 1) * tokens, :]


def place_kernel(lines, place_ref, *rest):
    pieces = rest[:lines]
    o_ref = rest[lines]
    width = pieces[0].shape[1]
    for s in range(lines):
        at = pl.multiple_of((place_ref[0] ^ s) * width, width)
        o_ref[:, pl.ds(at, width)] = pieces[s][...]


def grant(mebibytes):
    return pltpu.CompilerParams(vmem_limit_bytes=mebibytes * 2**20)


def on_chip(shape, dtype):
    return pltpu.VMEM(shape, dtype)


def near_core(x):
    return pltpu.with_memory_space_constraint(x, pltpu.VMEM)


def ordered(x, *before):
    return lax.optimization_barrier((x,) + before)[0]


def plane_body(lines, lanes):
    size = lines * lanes

    def hop(x, mask):
        return lax.ppermute(x, "ctx", [(c, c ^ mask) for c in range(size)])

    def swap(x):
        return lax.ppermute(x, "head", [(0, 1), (1, 0)])

    def spread(x, r):
        pairs = []
        for c in range(size):
            for h in range(2):
                block = (c // lanes) ^ r
                to = (2 * h + block // 2) * lanes + c % lanes
                pairs.append((2 * c + h, 2 * to + block % 2))
        return lax.ppermute(x, ("ctx", "head"), pairs)

    def plane_gather(pieces):
        one = [hop(p, 1) for p in pieces]
        two = [hop(p, 2) for p in pieces]
        three = []
        for s in range(len(pieces)):
            source, mask = (one[s], 2) if s % 2 == 0 else (two[s], 1)
            three.append(hop(source, mask))
        return (pieces, one, two, three)

    def inner(
        patches,
        patch_count,
        token_patch,
        window_ids,
        text_embed,
        vit_norm_gain,
        vit_qkv,
        vit_qkv_bias,
        vit_proj,
        vit_proj_bias,
        merge_norm_gain,
        merger,
        merger_bias,
        llm_norm_gain,
        w_qkv,
        qkv_bias,
    ):
        ctx_index = lax.axis_index("ctx")
        line = ctx_index // lanes
        lane = ctx_index % lanes
        side = lax.axis_index("head")
        tokens = patches.shape[0]
        own_cols = text_embed.shape[1]
        group_cols = (QH + 2) * HD
        mine = 2 * (line % 2) + side
        places = jnp.stack([line, lane, side, mine]).astype(jnp.int32)
        part_cols = own_cols // lines

        cut = pl.pallas_call(
            lambda *refs: cut_kernel(group_cols, *refs),
            out_shape=[on_chip((w_qkv.shape[0], group_cols), jnp.bfloat16)] * lines,
            in_specs=[smem_spec(), vmem_spec()],
            out_specs=[vmem_spec()] * lines,
            compiler_params=grant(8),
            name="cut",
        )(places, w_qkv)
        far_all = plane_gather([cut[0], hop(cut[2], lanes)])
        own_all = plane_gather([cut[1], hop(cut[3], lanes)])

        packed = pl.pallas_call(
            pack_kernel,
            out_shape=[on_chip((tokens + merger.shape[0] + 16, part_cols), jnp.bfloat16)] * lines,
            in_specs=[smem_spec()] + [vmem_spec()] * 4,
            out_specs=[vmem_spec()] * lines,
            compiler_params=grant(8),
            name="pack",
        )(places, text_embed, merger, token_patch.reshape(1, -1), merger_bias.reshape(1, -1))
        packed = [spread(x, r) for r, x in enumerate(packed)]
        span = slice(tokens, tokens + merger.shape[0])
        merger_own = jnp.concatenate([p[span] for p in packed], axis=0)
        merger_all = [merger_own] + [hop(merger_own, d) for d in range(1, lanes)]

        normed = rms_norm(patches, vit_norm_gain)
        attended = vision_heads(normed, vit_qkv, vit_qkv_bias, window_ids, patch_count[0], VHD)
        part = jnp.dot(attended, vit_proj, preferred_element_type=jnp.float32)
        part, places = lax.optimization_barrier((part, places))
        other_part = swap(part)
        vit_out = patches.astype(jnp.float32) + (part + other_part) + vit_proj_bias
        merged_in = rms_norm(vit_out, merge_norm_gain)
        share = tokens // 2
        merged_share = lax.dynamic_slice_in_dim(merged_in, side * share, share, 0)
        near = jnp.concatenate([hop(merged_share, s * lanes) for s in range(1, lines)], axis=0)
        far = swap(near)

        stitched = pl.pallas_call(
            lambda *refs: image_kernel(lines, lanes, *refs),
            out_shape=on_chip((lines * tokens, part_cols), jnp.bfloat16),
            in_specs=[smem_spec()] + [vmem_spec()] * (3 + lines + lanes),
            out_specs=vmem_spec(),
            scratch_shapes=[
                pltpu.VMEM((lines * tokens, merged_in.shape[1]), jnp.bfloat16),
                pltpu.VMEM((merger.shape[0] * size, part_cols), jnp.bfloat16),
            ],
            compiler_params=grant(24),
            name="image",
        )(places, merged_in, near, far, *packed, *merger_all)

        beside = swap(stitched)
        across = hop(stitched, lanes)
        both = swap(across)

        late = ordered(ctx_index, stitched)
        half = HD // 2
        steps = jnp.arange(half, dtype=jnp.float32) * (2.0 / HD)
        frequency = jnp.exp(-math.log(THETA) * steps)
        row = jnp.arange(lines * tokens, dtype=jnp.int32)
        positions = ((row // tokens) * lanes + late % lanes) * tokens
        positions = positions + row % tokens
        angle = positions.astype(jnp.float32)[:, None] * frequency[None, :]
        cosine = jnp.cos(angle)
        sine = jnp.sin(angle)
        cosine = jnp.concatenate([cosine, cosine], axis=-1)
        sine = jnp.concatenate([-sine, sine], axis=-1)

        gain = llm_norm_gain.reshape(1, -1)
        bias = qkv_bias.reshape(1, -1)
        depth = w_qkv.shape[0] * size
        rows = lines * tokens

        def collect(pieces):
            return pl.pallas_call(
                lambda *refs: collect_kernel(lanes, *refs),
                out_shape=on_chip((depth // 2, group_cols), jnp.bfloat16),
                in_specs=[smem_spec()] + [any_spec()] * (2 * lanes),
                out_specs=vmem_spec(),
                scratch_shapes=[pltpu.SemaphoreType.DMA((2 * lanes,))],
                compiler_params=grant(16),
                name="collect",
            )(places, *[pieces[d][e] for e in range(2) for d in range(lanes)])

        def product(kernel, weight, shapes, *operands):
            return pl.pallas_call(
                kernel,
                out_shape=shapes,
                in_specs=[smem_spec()] + [vmem_spec()] * (2 + len(operands)),
                out_specs=[vmem_spec()] * len(shapes),
                compiler_params=grant(28),
            )(places, gain, weight, *operands)

        far_weight = collect(far_all)
        own_weight = collect(own_all)
        sums, squares = product(
            lambda *refs: partial_kernel((0, 1), *refs),
            far_weight,
            [on_chip((rows, group_cols), jnp.float32), on_chip((rows, HD), jnp.float32)],
            stitched,
            beside,
        )
        last = (2, 3)
        send_kv, all_squares, square_row = product(
            lambda *refs: send_keys_kernel(last, *refs),
            far_weight,
            [
                on_chip((rows, 2 * HD), jnp.bfloat16),
                on_chip((rows, HD), jnp.float32),
                on_chip((8, rows), jnp.float32),
            ],
            across,
            both,
            sums,
            squares,
        )
        got_kv = hop(send_kv, 2 * lanes)
        got_row = hop(square_row, 2 * lanes)
        (send_q,) = product(
            lambda *refs: send_queries_kernel(last, *refs),
            far_weight,
            [on_chip((rows, QH * HD), jnp.bfloat16)],
            across,
            both,
            sums,
        )
        got_q = hop(send_q, 2 * lanes)
        (kept,) = product(
            lambda *refs: keep_kernel((0, 1, 2, 3), *refs),
            own_weight,
            [on_chip((rows, group_cols), jnp.float32)],
            stitched,
            beside,
            across,
            both,
        )
        closing = (bias, cosine, sine, places, all_squares, got_row, kept)
        closing_specs = [vmem_spec()] * 3 + [smem_spec()] + [vmem_spec()] * 4
        kv = pl.pallas_call(
            lambda *refs: key_kernel(depth, *refs),
            out_shape=on_chip((rows, 2 * HD), jnp.bfloat16),
            in_specs=closing_specs,
            out_specs=vmem_spec(),
            compiler_params=grant(24),
            name="keys",
        )(*closing, got_kv)
        kv_pieces = [kv] + [hop(kv, d) for d in range(1, lanes)]
        query = pl.pallas_call(
            lambda *refs: query_kernel(depth, *refs),
            out_shape=on_chip((lines, QH * tokens, HD), jnp.bfloat16),
            in_specs=closing_specs,
            out_specs=vmem_spec(),
            compiler_params=grant(24),
            name="queries",
        )(*closing, got_q)

        kv_all = pl.pallas_call(
            lambda *refs: gather_kernel(lines, lanes, *refs),
            out_shape=on_chip((size * tokens, 2 * HD), jnp.bfloat16),
            in_specs=[smem_spec()] + [vmem_spec()] * lanes,
            out_specs=vmem_spec(),
            compiler_params=grant(8),
            name="gather",
        )(places, *kv_pieces)

        def attend(which, kv_all):
            return pl.pallas_call(
                lambda *refs: attend_kernel(which, lanes, *refs),
                out_shape=[on_chip((tokens, QH * HD), jnp.bfloat16)] * len(which),
                in_specs=[smem_spec()] + [vmem_spec()] * 2,
                out_specs=[vmem_spec()] * len(which),
                compiler_params=grant(24),
                name="attend",
            )(places, kv_all, query)

        three, two = attend((3, 2), kv_all)
        (one,) = attend((1,), ordered(kv_all, three))
        (own,) = attend((0,), ordered(kv_all, one))
        three = hop(three, 3 * lanes)
        two = hop(two, 2 * lanes)
        one = hop(one, lanes)
        return pl.pallas_call(
            lambda *refs: place_kernel(lines, *refs),
            out_shape=jax.ShapeDtypeStruct((tokens, lines * QH * HD), jnp.bfloat16),
            in_specs=[smem_spec()] + [vmem_spec()] * lines,
            out_specs=vmem_spec(),
            compiler_params=grant(8),
            name="place",
        )(places, *[near_core(x) for x in (own, one, two, three)])

    return inner


def solution(mesh):
    specs = (
        P("ctx", None),
        P("ctx"),
        P("ctx"),
        P("ctx"),
        P("ctx", "head"),
        P(),
        P(None, "head"),
        P("head"),
        P("head", None),
        P(),
        P(),
        P("ctx", "head"),
        P("head"),
        P(),
        P("ctx", "head"),
        P("head"),
    )
    lines = KVH // mesh.shape["head"]
    lanes = mesh.shape["ctx"] // lines
    planes = mesh.shape["head"] == 2 and lines == 4 and lanes == 4
    body = plane_body(lines, lanes) if planes else general_body
    return jax.shard_map(
        body, mesh=mesh, in_specs=specs, out_specs=P("ctx", "head"), check_vma=False
    )
```

```python
import math

import jax
import jax.numpy as jnp
from jax import lax
from jax.experimental import pallas as pl
from jax.experimental.pallas import tpu as pltpu
from jax.sharding import PartitionSpec as P


VHD = 80
HD = 128
QH = 4
KVH = 8


EPSILON = 1e-06
THETA = 1000000.0
MASKED = -1e30


def rms_norm(rows, gain):
    values = rows.astype(jnp.float32)
    return (
        values * lax.rsqrt(jnp.mean(values * values, axis=-1, keepdims=True) + EPSILON) * gain
    ).astype(jnp.bfloat16)


def rotate(values, positions):
    head_size = values.shape[-1]
    half = head_size // 2
    steps = jnp.arange(half, dtype=jnp.float32) * (2.0 / head_size)
    frequency = jnp.exp(-math.log(THETA) * steps)
    angle = positions.astype(jnp.float32)[:, None] * frequency[None, :]
    cosine = jnp.cos(angle)[:, None, None, :]
    sine = jnp.sin(angle)[:, None, None, :]
    first = values[..., :half]
    second = values[..., half:]
    return jnp.concatenate(
        [first * cosine - second * sine, second * cosine + first * sine], axis=-1
    )


def vision_heads(normed, weight, bias, windows, count, head_size):
    slot_count = normed.shape[0]
    heads = weight.shape[1] // (3 * head_size)
    mixed = jnp.dot(normed, weight, preferred_element_type=jnp.float32) + bias
    mixed = mixed.astype(jnp.bfloat16).reshape(slot_count, heads, 3, head_size)
    return vision_weights(mixed, windows, count)


def vision_weights(mixed, windows, count):
    slot_count, heads, _, head_size = mixed.shape
    scores = jnp.einsum(
        "rhd,shd->hrs", mixed[:, :, 0], mixed[:, :, 1], preferred_element_type=jnp.float32
    ) * (1.0 / math.sqrt(head_size))
    index = jnp.arange(slot_count, dtype=jnp.int32)
    allowed = (windows[:, None] == windows[None, :]) & (
        (index[None, :] < count) | (index[:, None] == index[None, :])
    )
    scores = jnp.where(allowed[None], scores, MASKED)
    top = jnp.max(scores, axis=-1, keepdims=True)
    weights = jnp.where(allowed[None], jnp.exp(scores - top), 0.0)
    total = jnp.sum(weights, axis=-1)
    result = jnp.einsum(
        "hrs,shd->rhd",
        weights.astype(jnp.bfloat16),
        mixed[:, :, 2],
        preferred_element_type=jnp.float32,
    )
    return (
        (result / jnp.transpose(total)[:, :, None])
        .astype(jnp.bfloat16)
        .reshape(slot_count, heads * head_size)
    )


def attend_block(state, query, query_pos, key, value, key_pos, scale):
    top, total, summed_values = state
    scores = jnp.einsum("gjrd,sgd->gjrs", query, key, preferred_element_type=jnp.float32) * scale
    allowed = key_pos[None, :] <= query_pos[:, None]
    scores = jnp.where(allowed, scores, MASKED)
    new_top = jnp.maximum(top, jnp.max(scores, axis=-1))
    weights = jnp.where(allowed, jnp.exp(scores - new_top[..., None]), 0.0)
    factor = jnp.exp(top - new_top)
    total = total * factor + jnp.sum(weights, axis=-1)
    summed_values = summed_values * factor[..., None] + jnp.einsum(
        "gjrs,sgd->gjrd", weights.astype(jnp.bfloat16), value, preferred_element_type=jnp.float32
    )
    return (new_top, total, summed_values)


def visit_block(state, query, query_pos, key, value, key_pos, scale):
    return lax.cond(
        jnp.min(key_pos) <= jnp.max(query_pos),
        lambda inner: attend_block(inner, query, query_pos, key, value, key_pos, scale),
        lambda inner: inner,
        state,
    )


def general_body(
    patches,
    patch_count,
    token_patch,
    window_ids,
    text_embed,
    vit_norm_gain,
    vit_qkv,
    vit_qkv_bias,
    vit_proj,
    vit_proj_bias,
    merge_norm_gain,
    merger,
    merger_bias,
    llm_norm_gain,
    w_qkv,
    qkv_bias,
):
    ctx_index = lax.axis_index("ctx")
    tok_rows = patches.shape[0]
    half = tok_rows // 2
    normed = rms_norm(patches, vit_norm_gain)
    attended = vision_heads(normed, vit_qkv, vit_qkv_bias, window_ids, patch_count[0], VHD)
    partial_value = jnp.dot(attended, vit_proj, preferred_element_type=jnp.float32)
    summed = lax.psum_scatter(partial_value, "head", scatter_dimension=0, tiled=True)
    share_rows = summed.shape[0]
    own_rows = lax.dynamic_slice_in_dim(patches, lax.axis_index("head") * share_rows, share_rows, 0)
    vit_out = own_rows.astype(jnp.float32) + summed + vit_proj_bias
    merged_share = rms_norm(vit_out, merge_norm_gain)
    merged_in = lax.all_gather(merged_share, "head", axis=0, tiled=True)
    image_sum = jnp.dot(
        merged_in,
        lax.all_gather(merger, "ctx", axis=0, tiled=True),
        preferred_element_type=jnp.float32,
    )
    image = (image_sum + merger_bias).astype(jnp.bfloat16)
    picked = jnp.take(image, jnp.maximum(token_patch, 0), axis=0)
    stitched = jnp.where(token_patch[:, None] >= 0, picked, text_embed)
    whole = lax.all_gather(stitched, "head", axis=1, tiled=True)
    llm_in = rms_norm(whole, llm_norm_gain)
    projected = jnp.dot(
        llm_in, lax.all_gather(w_qkv, "ctx", axis=0, tiled=True), preferred_element_type=jnp.float32
    )
    projected = projected + qkv_bias
    groups = projected.shape[1] // ((QH + 2) * HD)
    projected = projected.reshape(tok_rows, groups, QH + 2, HD)
    positions = ctx_index * tok_rows + jnp.arange(tok_rows, dtype=jnp.int32)
    turned = rotate(projected[:, :, : QH + 1], positions).astype(jnp.bfloat16)
    queries = turned[:, :, :QH].reshape(tok_rows, groups * QH * HD)
    key_rows = turned[:, :, QH].reshape(tok_rows, groups * HD)
    value_rows = projected[:, :, QH + 1].astype(jnp.bfloat16).reshape(tok_rows, groups * HD)
    first_pos = ctx_index * tok_rows + jnp.arange(half, dtype=jnp.int32)
    second_pos = first_pos + half
    scale = 1.0 / math.sqrt(HD)
    query_heads = jnp.transpose(queries.reshape(tok_rows, groups, QH, HD), (1, 2, 0, 3))
    blocks = (query_heads[:, :, :half], query_heads[:, :, half:])
    block_pos = (first_pos, second_pos)

    def fresh():
        return (
            jnp.full((groups, QH, half), MASKED, jnp.float32),
            jnp.zeros((groups, QH, half), jnp.float32),
            jnp.zeros((groups, QH, half, HD), jnp.float32),
        )

    key_piece = lax.all_gather(key_rows, "ctx", axis=0, tiled=True)
    value_piece = lax.all_gather(value_rows, "ctx", axis=0, tiled=True)
    piece_rows = key_piece.shape[0]
    block_rows = math.gcd(piece_rows, tok_rows)
    block_count = piece_rows // block_rows
    key_piece = key_piece.reshape(block_count, block_rows, groups, HD)
    value_piece = value_piece.reshape(block_count, block_rows, groups, HD)

    def visit(index, states):
        key_block = lax.dynamic_index_in_dim(key_piece, index, 0, keepdims=False)
        value_block = lax.dynamic_index_in_dim(value_piece, index, 0, keepdims=False)
        row_index = index * block_rows + jnp.arange(block_rows, dtype=jnp.int32)
        updated = []
        for which in range(2):
            updated.append(
                visit_block(
                    states[which],
                    blocks[which],
                    block_pos[which],
                    key_block,
                    value_block,
                    row_index,
                    scale,
                )
            )
        return tuple(updated)

    carry = lax.fori_loop(0, block_count, visit, (fresh(), fresh()))
    outputs = []
    for state in carry:
        _, total, summed_values = state
        result = (summed_values / total[..., None]).astype(jnp.bfloat16)
        outputs.append(jnp.transpose(result, (2, 0, 1, 3)).reshape(half, groups * QH * HD))
    return jnp.concatenate(outputs, axis=0)


def any_spec():
    return pl.BlockSpec(memory_space=pl.ANY)


def vmem_spec():
    return pl.BlockSpec(memory_space=pltpu.VMEM)


def smem_spec():
    return pl.BlockSpec(memory_space=pltpu.SMEM)


def image_kernel(lines, lanes, place_ref, merged_ref, near_ref, far_ref, *rest):
    packed = rest[:lines]
    pieces = rest[lines : lines + lanes]
    out_ref, left, weight = rest[lines + lanes :]
    line = place_ref[0]
    lane = place_ref[1]
    side = place_ref[2]
    mine = place_ref[3]
    tokens = merged_ref.shape[0]
    share = tokens // 2
    rows = pieces[0].shape[0] // lines
    left[pl.ds(pl.multiple_of(line * tokens, tokens), tokens), :] = merged_ref[...]
    for s in range(1, lines):
        base = (line ^ s) * tokens
        near = pl.multiple_of(base + side * share, share)
        far = pl.multiple_of(base + (1 - side) * share, share)
        left[pl.ds(near, share), :] = near_ref[(s - 1) * share : s * share, :]
        left[pl.ds(far, share), :] = far_ref[(s - 1) * share : s * share, :]
    for d in range(lanes):
        for r in range(lines):
            block = (mine ^ r) * lanes + (lane ^ d)
            at = pl.multiple_of(block * rows, 16)
            weight[pl.ds(at, rows), :] = pieces[d][r * rows : (r + 1) * rows, :]
    extra = packed[0][tokens + rows : tokens + rows + 16, :].astype(jnp.float32)
    bias = extra[1:2, :] + extra[2:3, :] + extra[3:4, :]
    patch = lax.broadcasted_iota(jnp.int32, (tokens, tokens), 0).astype(jnp.float32)
    ones = jnp.ones((tokens, tokens), jnp.bfloat16)
    sublane = (((0,), (0,)), ((), ()))
    image = jnp.dot(left[...], weight[...], preferred_element_type=jnp.float32)
    left_image = (image + bias).astype(jnp.bfloat16)
    out_ref[...] = left_image
    for r in range(lines):
        at = pl.multiple_of((mine ^ r) * tokens, tokens)
        rows_image = out_ref[pl.ds(at, tokens), :]
        slots = packed[r][tokens + rows : tokens + rows + 16, :tokens].astype(jnp.float32)
        chosen = (patch == slots[:1, :]).astype(jnp.float32).astype(jnp.bfloat16)
        picked = lax.dot_general(chosen, rows_image, sublane, preferred_element_type=jnp.float32)
        found = lax.dot_general(chosen, ones, sublane, preferred_element_type=jnp.float32)
        out_ref[pl.ds(at, tokens), :] = jnp.where(
            found[:, :1] > 0.5, picked.astype(jnp.bfloat16), packed[r][:tokens, :]
        )


def cut_kernel(width, place_ref, w_ref, *outs):
    for s, o_ref in zip((2, 0, 3, 1), outs):
        at = pl.multiple_of((place_ref[0] ^ s) * width, width)
        o_ref[...] = w_ref[:, pl.ds(at, width)]


def pack_kernel(place_ref, text_ref, merger_ref, slot_ref, bias_ref, *outs):
    tokens = text_ref.shape[0]
    rows = merger_ref.shape[0]
    width = outs[0].shape[1]
    row = lax.broadcasted_iota(jnp.int32, (16, width), 0)
    slots = jnp.concatenate(
        [slot_ref[...].astype(jnp.float32), jnp.zeros((1, width - tokens), jnp.float32)], axis=1
    )
    for r, o_ref in enumerate(outs):
        cols = pl.ds(pl.multiple_of((place_ref[0] ^ r) * width, width), width)
        o_ref[:tokens, :] = text_ref[:, cols]
        o_ref[tokens : tokens + rows, :] = merger_ref[:, cols]
        bias = bias_ref[:, cols]
        high = bias.astype(jnp.bfloat16).astype(jnp.float32)
        middle = (bias - high).astype(jnp.bfloat16).astype(jnp.float32)
        low = bias - high - middle
        extra = jnp.where(row == 0, slots, 0.0)
        for at, value in ((1, high), (2, middle), (3, low)):
            extra = jnp.where(row == at, value, extra)
        o_ref[tokens + rows :, :] = extra.astype(jnp.bfloat16)


def vision_kernel(count_ref, patch_ref, gain_ref, w_ref, bias_ref, window_ref, proj_ref, out_ref):
    values = patch_ref[...].astype(jnp.float32)
    factor = lax.rsqrt(jnp.mean(values * values, axis=-1, keepdims=True) + EPSILON)
    normed = (values * factor * gain_ref[...]).astype(jnp.bfloat16)
    mixed = jnp.dot(normed, w_ref[...], preferred_element_type=jnp.float32) + bias_ref[...]
    mixed = mixed.astype(jnp.bfloat16)
    slots = patch_ref.shape[0]
    across = jnp.broadcast_to(window_ref[...].astype(jnp.float32), (slots, slots))
    column = lax.broadcasted_iota(jnp.int32, (slots, slots), 1)
    row = lax.broadcasted_iota(jnp.int32, (slots, slots), 0)
    allowed = (across == jnp.transpose(across)) & ((column < count_ref[0]) | (column == row))
    total_out = None
    for head in range(mixed.shape[1] // (3 * VHD)):
        at = head * 3 * VHD
        query = mixed[:, at : at + VHD]
        key = mixed[:, at + VHD : at + 2 * VHD]
        value = mixed[:, at + 2 * VHD : at + 3 * VHD]
        scores = lax.dot_general(
            query, key, (((1,), (1,)), ((), ())), preferred_element_type=jnp.float32
        ) * (1.0 / math.sqrt(VHD))
        scores = jnp.where(allowed, scores, MASKED)
        weights = jnp.exp(scores - jnp.max(scores, axis=-1, keepdims=True))
        total = jnp.sum(weights, axis=-1, keepdims=True)
        result = jnp.dot(weights.astype(jnp.bfloat16), value, preferred_element_type=jnp.float32)
        attended = (result / total).astype(jnp.bfloat16)
        product = jnp.dot(
            attended,
            proj_ref[head * VHD : (head + 1) * VHD, :],
            preferred_element_type=jnp.float32,
        )
        total_out = product if total_out is None else total_out + product
    out_ref[...] = total_out


def merge_kernel(place_ref, patch_ref, part_ref, other_ref, bias_ref, gain_ref, out_ref, share_ref):
    share = share_ref.shape[0]
    whole = patch_ref[...].astype(jnp.float32) + (part_ref[...] + other_ref[...]) + bias_ref[...]
    factor = lax.rsqrt(jnp.mean(whole * whole, axis=-1, keepdims=True) + EPSILON)
    merged = (whole * factor * gain_ref[...]).astype(jnp.bfloat16)
    out_ref[...] = merged
    at = pl.multiple_of(place_ref[2] * share, share)
    share_ref[...] = out_ref[pl.ds(at, share), :]


def collect_kernel(lanes, place_ref, *rest):
    pieces = rest[: 2 * lanes]
    w_ref, sems = rest[2 * lanes :]
    rows = pieces[0].shape[0]
    copies = []
    for e in range(2):
        for d in range(lanes):
            block = ((place_ref[0] % 2) ^ e) * lanes + (place_ref[1] ^ d)
            copies.append(
                pltpu.make_async_copy(
                    pieces[e * lanes + d],
                    w_ref.at[pl.ds(block * rows, rows), :],
                    sems.at[e * lanes + d],
                )
            )
    for copy in copies:
        copy.start()
    for copy in copies:
        copy.wait()


def add_blocks(blocks, pieces, cols, place_ref, gain_ref, w_ref, total):
    squares = None
    for e, piece in zip(blocks, pieces):
        width = piece.shape[1]
        at = pl.multiple_of((place_ref[3] ^ e) * width, width)
        depth = w_ref.shape[0]
        gain_at = pl.multiple_of((place_ref[0] // 2) * depth + at, width)
        rows = piece[...].astype(jnp.float32)
        more = jnp.sum(rows * rows, axis=-1, keepdims=True)
        squares = more if squares is None else squares + more
        scaled = (rows * gain_ref[:, pl.ds(gain_at, width)]).astype(jnp.bfloat16)
        product = jnp.dot(
            scaled, w_ref[pl.ds(at, width), cols], preferred_element_type=jnp.float32
        )
        total = product if total is None else total + product
    return total, squares


def partial_kernel(blocks, place_ref, gain_ref, w_ref, *rest):
    pieces = rest[: len(blocks)]
    sum_ref, square_ref = rest[len(blocks) :]
    total, squares = add_blocks(
        blocks, pieces, slice(0, w_ref.shape[1]), place_ref, gain_ref, w_ref, None
    )
    sum_ref[...] = total
    square_ref[...] = jnp.broadcast_to(squares, square_ref.shape)


def send_keys_kernel(blocks, place_ref, gain_ref, w_ref, *rest):
    pieces = rest[: len(blocks)]
    sum_ref, square_ref, out_ref, all_ref, row_ref = rest[len(blocks) :]
    cols = slice(QH * HD, w_ref.shape[1])
    total, squares = add_blocks(
        blocks, pieces, cols, place_ref, gain_ref, w_ref, sum_ref[:, cols]
    )
    out_ref[...] = total.astype(jnp.bfloat16)
    squares = square_ref[...] + jnp.broadcast_to(squares, square_ref.shape)
    all_ref[...] = squares
    row_ref[...] = jnp.transpose(squares)[: row_ref.shape[0], :]


def send_queries_kernel(blocks, place_ref, gain_ref, w_ref, *rest):
    pieces = rest[: len(blocks)]
    sum_ref, far_ref, near_ref, whole = rest[len(blocks) :]
    cols = slice(0, QH * HD)
    total, _ = add_blocks(blocks, pieces, cols, place_ref, gain_ref, w_ref, sum_ref[:, cols])
    whole[...] = total.astype(jnp.bfloat16)
    rows = far_ref.shape[0]
    half = place_ref[0] // 2
    far_ref[...] = whole[pl.ds(pl.multiple_of(half * rows, rows), rows), :]
    near_ref[...] = whole[pl.ds(pl.multiple_of((1 - half) * rows, rows), rows), :]


def keep_kernel(blocks, place_ref, gain_ref, w_ref, *rest):
    pieces = rest[: len(blocks)]
    out_ref = rest[len(blocks)]
    cols = slice(0, w_ref.shape[1])
    out_ref[...] = add_blocks(blocks, pieces, cols, place_ref, gain_ref, w_ref, None)[0]


def row_factor(depth, all_ref, row_ref):
    rows = jnp.broadcast_to(row_ref[:1, :], (all_ref.shape[1], row_ref.shape[1]))
    squares = all_ref[...] + jnp.transpose(rows)
    return lax.rsqrt(squares / depth + EPSILON)


def turn(x, cosine, sine):
    return x * cosine + pltpu.roll(x, x.shape[1] // 2, 1) * sine


def key_kernel(depth, bias_ref, cos_ref, sin_ref, place_ref, all_ref, row_ref, *rest):
    keep_ref, got_ref, kv_ref = rest
    factor = row_factor(depth, all_ref, row_ref)
    group = keep_ref.shape[1]
    at = pl.multiple_of(place_ref[0] * group + QH * HD, HD)
    total = keep_ref[:, QH * HD :] + got_ref[...].astype(jnp.float32)
    key = total[:, :HD] * factor + bias_ref[:, pl.ds(at, HD)]
    value = total[:, HD:] * factor + bias_ref[:, pl.ds(at + HD, HD)]
    kv_ref[:, :HD] = turn(key, cos_ref[...], sin_ref[...]).astype(jnp.bfloat16)
    kv_ref[:, HD:] = value.astype(jnp.bfloat16)


def query_kernel(depth, far, bias_ref, cos_ref, sin_ref, place_ref, all_ref, row_ref, *rest):
    keep_ref, got_ref, q_ref, factors = rest
    lines, _, _ = q_ref.shape
    rows = got_ref.shape[0]
    tokens = rows // lines
    factors[...] = row_factor(depth, all_ref, row_ref)
    half = place_ref[0] // 2
    half = 1 - half if far else half
    mine = pl.ds(pl.multiple_of(half * rows, rows), rows)
    factor = factors[mine, :]
    cosine = cos_ref[mine, :]
    sine = sin_ref[mine, :]
    group = keep_ref.shape[1]
    for j in range(QH):
        cols = slice(j * HD, (j + 1) * HD)
        at = pl.multiple_of(place_ref[0] * group + j * HD, HD)
        total = keep_ref[mine, cols] + got_ref[:, cols].astype(jnp.float32)
        head = turn(total * factor + bias_ref[:, pl.ds(at, HD)], cosine, sine)
        head = head.astype(jnp.bfloat16)
        for s in range(lines):
            q_ref[s, j * tokens : (j + 1) * tokens, :] = head[s * tokens : (s + 1) * tokens, :]


def gather_kernel(lines, lanes, place_ref, *rest):
    pieces = rest[:lanes]
    kv_ref = rest[lanes]
    tokens = kv_ref.shape[0] // (lines * lanes)
    for d in range(lanes):
        for z in range(lines):
            at = pl.multiple_of((z * lanes + (place_ref[1] ^ d)) * tokens, tokens)
            kv_ref[pl.ds(at, tokens), :] = pieces[d][z * tokens : (z + 1) * tokens, :]


def attend_kernel(which, lanes, place_ref, kv, q_ref, *outs):
    tokens = outs[0].shape[0]
    lane = place_ref[1]
    span = lanes * tokens
    scale = 1.0 / math.sqrt(HD)
    rows = QH * tokens
    row_pos = lane * tokens + lax.rem(lax.broadcasted_iota(jnp.int32, (rows, span), 0), tokens)
    visible = lax.broadcasted_iota(jnp.int32, (rows, span), 1) <= row_pos

    for o_ref, s in zip(outs, which):
        query = q_ref[(place_ref[0] ^ s) % q_ref.shape[0]]

        def visit(chunk, state, masked):
            top, total, summed = state
            at = pl.multiple_of(chunk * span, span)
            key = kv[pl.ds(at, span), :HD]
            value = kv[pl.ds(at, span), HD:]
            scores = (
                lax.dot_general(
                    query, key, (((1,), (1,)), ((), ())), preferred_element_type=jnp.float32
                )
                * scale
            )
            if masked:
                scores = jnp.where(visible, scores, MASKED)
            new_top = jnp.maximum(top, jnp.max(scores, axis=-1, keepdims=True))
            weights = jnp.exp(scores - new_top)
            factor = jnp.exp(top - new_top)
            total = total * factor + jnp.sum(weights, axis=-1, keepdims=True)
            summed = summed * factor + jnp.dot(
                weights.astype(jnp.bfloat16), value, preferred_element_type=jnp.float32
            )
            return new_top, total, summed

        line = place_ref[0] ^ s
        state = (
            jnp.full((rows, 1), MASKED, jnp.float32),
            jnp.zeros((rows, 1), jnp.float32),
            jnp.zeros((rows, HD), jnp.float32),
        )
        state = visit(line, state, True)
        state = lax.fori_loop(0, line, lambda c, st: visit(c, st, False), state)
        _, total, summed = state
        result = (summed / total).astype(jnp.bfloat16)
        for j in range(QH):
            o_ref[:, j * HD : (j + 1) * HD] = result[j * tokens : (j + 1) * tokens, :]


def place_kernel(lines, place_ref, *rest):
    pieces = rest[:lines]
    o_ref = rest[lines]
    width = pieces[0].shape[1]
    for s in range(lines):
        at = pl.multiple_of((place_ref[0] ^ s) * width, width)
        o_ref[:, pl.ds(at, width)] = pieces[s][...]


def grant(mebibytes):
    return pltpu.CompilerParams(vmem_limit_bytes=mebibytes * 2**20)


def on_chip(shape, dtype):
    return pltpu.VMEM(shape, dtype)


def near_core(x):
    return pltpu.with_memory_space_constraint(x, pltpu.VMEM)


def far_core(x):
    return pltpu.with_memory_space_constraint(x, pltpu.HBM)


def ordered(x, *before):
    return lax.optimization_barrier((x,) + before)[0]


def plane_body(lines, lanes):
    size = lines * lanes

    def hop(x, mask):
        return lax.ppermute(x, "ctx", [(c, c ^ mask) for c in range(size)])

    def swap(x):
        return lax.ppermute(x, "head", [(0, 1), (1, 0)])

    def spread(x, r):
        pairs = []
        for c in range(size):
            for h in range(2):
                block = (c // lanes) ^ r
                to = (2 * h + block // 2) * lanes + c % lanes
                pairs.append((2 * c + h, 2 * to + block % 2))
        return lax.ppermute(x, ("ctx", "head"), pairs)

    def plane_gather(pieces):
        one = [hop(p, 1) for p in pieces]
        two = [hop(p, 2) for p in pieces]
        three = []
        for s in range(len(pieces)):
            source, mask = (one[s], 2) if s % 2 == 0 else (two[s], 1)
            three.append(hop(source, mask))
        return (pieces, one, two, three)

    def inner(
        patches,
        patch_count,
        token_patch,
        window_ids,
        text_embed,
        vit_norm_gain,
        vit_qkv,
        vit_qkv_bias,
        vit_proj,
        vit_proj_bias,
        merge_norm_gain,
        merger,
        merger_bias,
        llm_norm_gain,
        w_qkv,
        qkv_bias,
    ):
        ctx_index = lax.axis_index("ctx")
        line = ctx_index // lanes
        lane = ctx_index % lanes
        side = lax.axis_index("head")
        tokens = patches.shape[0]
        own_cols = text_embed.shape[1]
        group_cols = (QH + 2) * HD
        mine = 2 * (line % 2) + side
        places = jnp.stack([line, lane, side, mine]).astype(jnp.int32)
        part_cols = own_cols // lines

        cut = pl.pallas_call(
            lambda *refs: cut_kernel(group_cols, *refs),
            out_shape=[on_chip((w_qkv.shape[0], group_cols), jnp.bfloat16)] * lines,
            in_specs=[smem_spec(), vmem_spec()],
            out_specs=[vmem_spec()] * lines,
            compiler_params=grant(8),
            name="cut",
        )(places, far_core(w_qkv))
        far_all = plane_gather([cut[0], hop(cut[2], lanes)])
        own_all = plane_gather([cut[1], hop(cut[3], lanes)])

        packed = pl.pallas_call(
            pack_kernel,
            out_shape=[on_chip((tokens + merger.shape[0] + 16, part_cols), jnp.bfloat16)] * lines,
            in_specs=[smem_spec()] + [vmem_spec()] * 4,
            out_specs=[vmem_spec()] * lines,
            compiler_params=grant(8),
            name="pack",
        )(
            places,
            far_core(text_embed),
            far_core(merger),
            far_core(token_patch.reshape(1, -1)),
            far_core(merger_bias.reshape(1, -1)),
        )
        packed = [spread(x, r) for r, x in enumerate(packed)]
        span = slice(tokens, tokens + merger.shape[0])
        merger_own = jnp.concatenate([p[span] for p in packed], axis=0)
        merger_all = [merger_own] + [hop(merger_own, d) for d in range(1, lanes)]

        width = patches.shape[1]
        part = pl.pallas_call(
            vision_kernel,
            out_shape=on_chip((tokens, width), jnp.float32),
            in_specs=[smem_spec()] + [vmem_spec()] * 6,
            out_specs=vmem_spec(),
            compiler_params=grant(24),
            name="vision",
        )(
            patch_count,
            far_core(patches),
            far_core(vit_norm_gain.reshape(1, -1)),
            far_core(vit_qkv),
            far_core(vit_qkv_bias.reshape(1, -1)),
            far_core(window_ids.reshape(1, -1)),
            near_core(vit_proj),
        )
        other_part = swap(part)
        merged_in, merged_share = pl.pallas_call(
            merge_kernel,
            out_shape=[
                on_chip((tokens, width), jnp.bfloat16),
                on_chip((tokens // 2, width), jnp.bfloat16),
            ],
            in_specs=[smem_spec()] + [vmem_spec()] * 5,
            out_specs=[vmem_spec()] * 2,
            compiler_params=grant(12),
            name="merge",
        )(
            places,
            patches,
            part,
            other_part,
            vit_proj_bias.reshape(1, -1),
            merge_norm_gain.reshape(1, -1),
        )
        near = jnp.concatenate([hop(merged_share, s * lanes) for s in range(1, lines)], axis=0)
        far = swap(near)

        stitched = pl.pallas_call(
            lambda *refs: image_kernel(lines, lanes, *refs),
            out_shape=on_chip((lines * tokens, part_cols), jnp.bfloat16),
            in_specs=[smem_spec()] + [vmem_spec()] * (3 + lines + lanes),
            out_specs=vmem_spec(),
            scratch_shapes=[
                pltpu.VMEM((lines * tokens, merged_in.shape[1]), jnp.bfloat16),
                pltpu.VMEM((merger.shape[0] * size, part_cols), jnp.bfloat16),
            ],
            compiler_params=grant(24),
            name="image",
        )(places, merged_in, near, far, *packed, *merger_all)

        beside = swap(stitched)
        across = hop(stitched, lanes)
        both = swap(across)

        late = ordered(ctx_index, stitched)
        half = HD // 2
        steps = jnp.arange(half, dtype=jnp.float32) * (2.0 / HD)
        frequency = jnp.exp(-math.log(THETA) * steps)
        row = jnp.arange(lines * tokens, dtype=jnp.int32)
        positions = ((row // tokens) * lanes + late % lanes) * tokens
        positions = positions + row % tokens
        angle = positions.astype(jnp.float32)[:, None] * frequency[None, :]
        cosine = jnp.cos(angle)
        sine = jnp.sin(angle)
        cosine = jnp.concatenate([cosine, cosine], axis=-1)
        sine = jnp.concatenate([-sine, sine], axis=-1)

        gain = llm_norm_gain.reshape(1, -1)
        bias = qkv_bias.reshape(1, -1)
        depth = w_qkv.shape[0] * size
        rows = lines * tokens

        def collect(pieces):
            return pl.pallas_call(
                lambda *refs: collect_kernel(lanes, *refs),
                out_shape=on_chip((depth // 2, group_cols), jnp.bfloat16),
                in_specs=[smem_spec()] + [any_spec()] * (2 * lanes),
                out_specs=vmem_spec(),
                scratch_shapes=[pltpu.SemaphoreType.DMA((2 * lanes,))],
                compiler_params=grant(16),
                name="collect",
            )(places, *[pieces[d][e] for e in range(2) for d in range(lanes)])

        def product(kernel, weight, shapes, *operands, scratch=()):
            return pl.pallas_call(
                kernel,
                out_shape=shapes,
                in_specs=[smem_spec()] + [vmem_spec()] * (2 + len(operands)),
                out_specs=[vmem_spec()] * len(shapes),
                scratch_shapes=list(scratch),
                compiler_params=grant(28),
            )(places, gain, weight, *operands)

        far_weight = collect(far_all)
        own_weight = collect(own_all)
        sums, squares = product(
            lambda *refs: partial_kernel((0, 1), *refs),
            far_weight,
            [on_chip((rows, group_cols), jnp.float32), on_chip((rows, HD), jnp.float32)],
            stitched,
            beside,
        )
        last = (2, 3)
        send_kv, all_squares, square_row = product(
            lambda *refs: send_keys_kernel(last, *refs),
            far_weight,
            [
                on_chip((rows, 2 * HD), jnp.bfloat16),
                on_chip((rows, HD), jnp.float32),
                on_chip((8, rows), jnp.float32),
            ],
            across,
            both,
            sums,
            squares,
        )
        got_kv = hop(send_kv, 2 * lanes)
        got_row = hop(square_row, 2 * lanes)
        send_far, send_near = product(
            lambda *refs: send_queries_kernel(last, *refs),
            far_weight,
            [on_chip((rows // 2, QH * HD), jnp.bfloat16)] * 2,
            across,
            both,
            sums,
            scratch=[pltpu.VMEM((rows, QH * HD), jnp.bfloat16)],
        )
        got_far = hop(send_far, 2 * lanes)
        got_near = hop(send_near, 2 * lanes)
        (kept,) = product(
            lambda *refs: keep_kernel((0, 1, 2, 3), *refs),
            own_weight,
            [on_chip((rows, group_cols), jnp.float32)],
            stitched,
            beside,
            across,
            both,
        )
        closing = (bias, cosine, sine, places, all_squares, got_row, kept)
        closing_specs = [vmem_spec()] * 3 + [smem_spec()] + [vmem_spec()] * 4
        kv = pl.pallas_call(
            lambda *refs: key_kernel(depth, *refs),
            out_shape=on_chip((rows, 2 * HD), jnp.bfloat16),
            in_specs=closing_specs,
            out_specs=vmem_spec(),
            compiler_params=grant(24),
            name="keys",
        )(*closing, got_kv)
        kv_pieces = [kv] + [hop(kv, d) for d in range(1, lanes)]

        def queries_of(far, got):
            return pl.pallas_call(
                lambda *refs: query_kernel(depth, far, *refs),
                out_shape=on_chip((lines // 2, QH * tokens, HD), jnp.bfloat16),
                in_specs=closing_specs,
                out_specs=vmem_spec(),
                scratch_shapes=[pltpu.VMEM((rows, HD), jnp.float32)],
                compiler_params=grant(24),
                name="queries",
            )(*closing, got)

        query_far = queries_of(True, got_far)
        kv_all = pl.pallas_call(
            lambda *refs: gather_kernel(lines, lanes, *refs),
            out_shape=on_chip((size * tokens, 2 * HD), jnp.bfloat16),
            in_specs=[smem_spec()] + [vmem_spec()] * lanes,
            out_specs=vmem_spec(),
            compiler_params=grant(8),
            name="gather",
        )(places, *kv_pieces)

        def attend(which, kv_all, query):
            return pl.pallas_call(
                lambda *refs: attend_kernel(which, lanes, *refs),
                out_shape=[on_chip((tokens, QH * HD), jnp.bfloat16)] * len(which),
                in_specs=[smem_spec()] + [vmem_spec()] * 2,
                out_specs=[vmem_spec()] * len(which),
                compiler_params=grant(24),
                name="attend",
            )(places, kv_all, query)

        three, two = attend((3, 2), kv_all, query_far)
        query_near = queries_of(False, ordered(got_near, three))
        (one,) = attend((1,), kv_all, query_near)
        (own,) = attend((0,), ordered(kv_all, one), query_near)
        three = hop(three, 3 * lanes)
        two = hop(two, 2 * lanes)
        one = hop(one, lanes)
        return pl.pallas_call(
            lambda *refs: place_kernel(lines, *refs),
            out_shape=jax.ShapeDtypeStruct((tokens, lines * QH * HD), jnp.bfloat16),
            in_specs=[smem_spec()] + [vmem_spec()] * lines,
            out_specs=vmem_spec(),
            compiler_params=grant(8),
            name="place",
        )(places, *[near_core(x) for x in (own, one, two, three)])

    return inner


def solution(mesh):
    specs = (
        P("ctx", None),
        P("ctx"),
        P("ctx"),
        P("ctx"),
        P("ctx", "head"),
        P(),
        P(None, "head"),
        P("head"),
        P("head", None),
        P(),
        P(),
        P("ctx", "head"),
        P("head"),
        P(),
        P("ctx", "head"),
        P("head"),
    )
    lines = KVH // mesh.shape["head"]
    lanes = mesh.shape["ctx"] // lines
    planes = mesh.shape["head"] == 2 and lines == 4 and lanes == 4
    body = plane_body(lines, lanes) if planes else general_body
    return jax.shard_map(
        body, mesh=mesh, in_specs=specs, out_specs=P("ctx", "head"), check_vma=False
    )
```

```python
import math

import jax
import jax.numpy as jnp
from jax import lax
from jax.experimental import pallas as pl
from jax.experimental.pallas import tpu as pltpu
from jax.sharding import PartitionSpec as P


VHD = 80
HD = 128
QH = 4
KVH = 8


EPSILON = 1e-06
THETA = 1000000.0
MASKED = -1e30


def rms_norm(rows, gain):
    values = rows.astype(jnp.float32)
    return (
        values * lax.rsqrt(jnp.mean(values * values, axis=-1, keepdims=True) + EPSILON) * gain
    ).astype(jnp.bfloat16)


def rotate(values, positions):
    head_size = values.shape[-1]
    half = head_size // 2
    steps = jnp.arange(half, dtype=jnp.float32) * (2.0 / head_size)
    frequency = jnp.exp(-math.log(THETA) * steps)
    angle = positions.astype(jnp.float32)[:, None] * frequency[None, :]
    cosine = jnp.cos(angle)[:, None, None, :]
    sine = jnp.sin(angle)[:, None, None, :]
    first = values[..., :half]
    second = values[..., half:]
    return jnp.concatenate(
        [first * cosine - second * sine, second * cosine + first * sine], axis=-1
    )


def vision_heads(normed, weight, bias, windows, count, head_size):
    slot_count = normed.shape[0]
    heads = weight.shape[1] // (3 * head_size)
    mixed = jnp.dot(normed, weight, preferred_element_type=jnp.float32) + bias
    mixed = mixed.astype(jnp.bfloat16).reshape(slot_count, heads, 3, head_size)
    return vision_weights(mixed, windows, count)


def vision_weights(mixed, windows, count):
    slot_count, heads, _, head_size = mixed.shape
    scores = jnp.einsum(
        "rhd,shd->hrs", mixed[:, :, 0], mixed[:, :, 1], preferred_element_type=jnp.float32
    ) * (1.0 / math.sqrt(head_size))
    index = jnp.arange(slot_count, dtype=jnp.int32)
    allowed = (windows[:, None] == windows[None, :]) & (
        (index[None, :] < count) | (index[:, None] == index[None, :])
    )
    scores = jnp.where(allowed[None], scores, MASKED)
    top = jnp.max(scores, axis=-1, keepdims=True)
    weights = jnp.where(allowed[None], jnp.exp(scores - top), 0.0)
    total = jnp.sum(weights, axis=-1)
    result = jnp.einsum(
        "hrs,shd->rhd",
        weights.astype(jnp.bfloat16),
        mixed[:, :, 2],
        preferred_element_type=jnp.float32,
    )
    return (
        (result / jnp.transpose(total)[:, :, None])
        .astype(jnp.bfloat16)
        .reshape(slot_count, heads * head_size)
    )


def attend_block(state, query, query_pos, key, value, key_pos, scale):
    top, total, summed_values = state
    scores = jnp.einsum("gjrd,sgd->gjrs", query, key, preferred_element_type=jnp.float32) * scale
    allowed = key_pos[None, :] <= query_pos[:, None]
    scores = jnp.where(allowed, scores, MASKED)
    new_top = jnp.maximum(top, jnp.max(scores, axis=-1))
    weights = jnp.where(allowed, jnp.exp(scores - new_top[..., None]), 0.0)
    factor = jnp.exp(top - new_top)
    total = total * factor + jnp.sum(weights, axis=-1)
    summed_values = summed_values * factor[..., None] + jnp.einsum(
        "gjrs,sgd->gjrd", weights.astype(jnp.bfloat16), value, preferred_element_type=jnp.float32
    )
    return (new_top, total, summed_values)


def visit_block(state, query, query_pos, key, value, key_pos, scale):
    return lax.cond(
        jnp.min(key_pos) <= jnp.max(query_pos),
        lambda inner: attend_block(inner, query, query_pos, key, value, key_pos, scale),
        lambda inner: inner,
        state,
    )


def general_body(
    patches,
    patch_count,
    token_patch,
    window_ids,
    text_embed,
    vit_norm_gain,
    vit_qkv,
    vit_qkv_bias,
    vit_proj,
    vit_proj_bias,
    merge_norm_gain,
    merger,
    merger_bias,
    llm_norm_gain,
    w_qkv,
    qkv_bias,
):
    ctx_index = lax.axis_index("ctx")
    tok_rows = patches.shape[0]
    half = tok_rows // 2
    normed = rms_norm(patches, vit_norm_gain)
    attended = vision_heads(normed, vit_qkv, vit_qkv_bias, window_ids, patch_count[0], VHD)
    partial_value = jnp.dot(attended, vit_proj, preferred_element_type=jnp.float32)
    summed = lax.psum_scatter(partial_value, "head", scatter_dimension=0, tiled=True)
    share_rows = summed.shape[0]
    own_rows = lax.dynamic_slice_in_dim(patches, lax.axis_index("head") * share_rows, share_rows, 0)
    vit_out = own_rows.astype(jnp.float32) + summed + vit_proj_bias
    merged_share = rms_norm(vit_out, merge_norm_gain)
    merged_in = lax.all_gather(merged_share, "head", axis=0, tiled=True)
    image_sum = jnp.dot(
        merged_in,
        lax.all_gather(merger, "ctx", axis=0, tiled=True),
        preferred_element_type=jnp.float32,
    )
    image = (image_sum + merger_bias).astype(jnp.bfloat16)
    picked = jnp.take(image, jnp.maximum(token_patch, 0), axis=0)
    stitched = jnp.where(token_patch[:, None] >= 0, picked, text_embed)
    whole = lax.all_gather(stitched, "head", axis=1, tiled=True)
    llm_in = rms_norm(whole, llm_norm_gain)
    projected = jnp.dot(
        llm_in, lax.all_gather(w_qkv, "ctx", axis=0, tiled=True), preferred_element_type=jnp.float32
    )
    projected = projected + qkv_bias
    groups = projected.shape[1] // ((QH + 2) * HD)
    projected = projected.reshape(tok_rows, groups, QH + 2, HD)
    positions = ctx_index * tok_rows + jnp.arange(tok_rows, dtype=jnp.int32)
    turned = rotate(projected[:, :, : QH + 1], positions).astype(jnp.bfloat16)
    queries = turned[:, :, :QH].reshape(tok_rows, groups * QH * HD)
    key_rows = turned[:, :, QH].reshape(tok_rows, groups * HD)
    value_rows = projected[:, :, QH + 1].astype(jnp.bfloat16).reshape(tok_rows, groups * HD)
    first_pos = ctx_index * tok_rows + jnp.arange(half, dtype=jnp.int32)
    second_pos = first_pos + half
    scale = 1.0 / math.sqrt(HD)
    query_heads = jnp.transpose(queries.reshape(tok_rows, groups, QH, HD), (1, 2, 0, 3))
    blocks = (query_heads[:, :, :half], query_heads[:, :, half:])
    block_pos = (first_pos, second_pos)

    def fresh():
        return (
            jnp.full((groups, QH, half), MASKED, jnp.float32),
            jnp.zeros((groups, QH, half), jnp.float32),
            jnp.zeros((groups, QH, half, HD), jnp.float32),
        )

    key_piece = lax.all_gather(key_rows, "ctx", axis=0, tiled=True)
    value_piece = lax.all_gather(value_rows, "ctx", axis=0, tiled=True)
    piece_rows = key_piece.shape[0]
    block_rows = math.gcd(piece_rows, tok_rows)
    block_count = piece_rows // block_rows
    key_piece = key_piece.reshape(block_count, block_rows, groups, HD)
    value_piece = value_piece.reshape(block_count, block_rows, groups, HD)

    def visit(index, states):
        key_block = lax.dynamic_index_in_dim(key_piece, index, 0, keepdims=False)
        value_block = lax.dynamic_index_in_dim(value_piece, index, 0, keepdims=False)
        row_index = index * block_rows + jnp.arange(block_rows, dtype=jnp.int32)
        updated = []
        for which in range(2):
            updated.append(
                visit_block(
                    states[which],
                    blocks[which],
                    block_pos[which],
                    key_block,
                    value_block,
                    row_index,
                    scale,
                )
            )
        return tuple(updated)

    carry = lax.fori_loop(0, block_count, visit, (fresh(), fresh()))
    outputs = []
    for state in carry:
        _, total, summed_values = state
        result = (summed_values / total[..., None]).astype(jnp.bfloat16)
        outputs.append(jnp.transpose(result, (2, 0, 1, 3)).reshape(half, groups * QH * HD))
    return jnp.concatenate(outputs, axis=0)


def any_spec():
    return pl.BlockSpec(memory_space=pl.ANY)


def vmem_spec():
    return pl.BlockSpec(memory_space=pltpu.VMEM)


def smem_spec():
    return pl.BlockSpec(memory_space=pltpu.SMEM)


def image_kernel(lines, lanes, place_ref, merged_ref, near_ref, far_ref, *rest):
    packed = rest[:lines]
    pieces = rest[lines : lines + lanes]
    out_ref, left, weight = rest[lines + lanes :]
    line = place_ref[0]
    lane = place_ref[1]
    side = place_ref[2]
    mine = place_ref[3]
    tokens = merged_ref.shape[0]
    share = tokens // 2
    rows = pieces[0].shape[0] // lines
    left[pl.ds(pl.multiple_of(line * tokens, tokens), tokens), :] = merged_ref[...]
    for s in range(1, lines):
        base = (line ^ s) * tokens
        near = pl.multiple_of(base + side * share, share)
        far = pl.multiple_of(base + (1 - side) * share, share)
        left[pl.ds(near, share), :] = near_ref[(s - 1) * share : s * share, :]
        left[pl.ds(far, share), :] = far_ref[(s - 1) * share : s * share, :]
    for d in range(lanes):
        for r in range(lines):
            block = (mine ^ r) * lanes + (lane ^ d)
            at = pl.multiple_of(block * rows, 16)
            weight[pl.ds(at, rows), :] = pieces[d][r * rows : (r + 1) * rows, :]
    extra = packed[0][tokens + rows : tokens + rows + 16, :].astype(jnp.float32)
    bias = extra[1:2, :] + extra[2:3, :] + extra[3:4, :]
    patch = lax.broadcasted_iota(jnp.int32, (tokens, tokens), 0).astype(jnp.float32)
    ones = jnp.ones((tokens, tokens), jnp.bfloat16)
    sublane = (((0,), (0,)), ((), ()))
    image = jnp.dot(left[...], weight[...], preferred_element_type=jnp.float32)
    left_image = (image + bias).astype(jnp.bfloat16)
    out_ref[...] = left_image
    for r in range(lines):
        at = pl.multiple_of((mine ^ r) * tokens, tokens)
        rows_image = out_ref[pl.ds(at, tokens), :]
        slots = packed[r][tokens + rows : tokens + rows + 16, :tokens].astype(jnp.float32)
        chosen = (patch == slots[:1, :]).astype(jnp.float32).astype(jnp.bfloat16)
        picked = lax.dot_general(chosen, rows_image, sublane, preferred_element_type=jnp.float32)
        found = lax.dot_general(chosen, ones, sublane, preferred_element_type=jnp.float32)
        out_ref[pl.ds(at, tokens), :] = jnp.where(
            found[:, :1] > 0.5, picked.astype(jnp.bfloat16), packed[r][:tokens, :]
        )


def cut_kernel(width, place_ref, w_ref, *outs):
    for s, o_ref in zip((2, 0, 3, 1), outs):
        at = pl.multiple_of((place_ref[0] ^ s) * width, width)
        o_ref[...] = w_ref[:, pl.ds(at, width)]


def pack_kernel(place_ref, text_ref, merger_ref, slot_ref, bias_ref, *outs):
    tokens = text_ref.shape[0]
    rows = merger_ref.shape[0]
    width = outs[0].shape[1]
    row = lax.broadcasted_iota(jnp.int32, (16, width), 0)
    slots = jnp.concatenate(
        [slot_ref[...].astype(jnp.float32), jnp.zeros((1, width - tokens), jnp.float32)], axis=1
    )
    for r, o_ref in enumerate(outs):
        cols = pl.ds(pl.multiple_of((place_ref[0] ^ r) * width, width), width)
        o_ref[:tokens, :] = text_ref[:, cols]
        o_ref[tokens : tokens + rows, :] = merger_ref[:, cols]
        bias = bias_ref[:, cols]
        high = bias.astype(jnp.bfloat16).astype(jnp.float32)
        middle = (bias - high).astype(jnp.bfloat16).astype(jnp.float32)
        low = bias - high - middle
        extra = jnp.where(row == 0, slots, 0.0)
        for at, value in ((1, high), (2, middle), (3, low)):
            extra = jnp.where(row == at, value, extra)
        o_ref[tokens + rows :, :] = extra.astype(jnp.bfloat16)


def vision_kernel(count_ref, patch_ref, gain_ref, w_ref, bias_ref, window_ref, proj_ref, out_ref):
    values = patch_ref[...].astype(jnp.float32)
    factor = lax.rsqrt(jnp.mean(values * values, axis=-1, keepdims=True) + EPSILON)
    normed = (values * factor * gain_ref[...].reshape(1, -1)).astype(jnp.bfloat16)
    mixed = jnp.dot(normed, w_ref[...], preferred_element_type=jnp.float32) + bias_ref[...].reshape(1, -1)
    mixed = mixed.astype(jnp.bfloat16)
    slots = patch_ref.shape[0]
    across = jnp.broadcast_to(window_ref[...].astype(jnp.float32), (slots, slots))
    column = lax.broadcasted_iota(jnp.int32, (slots, slots), 1)
    row = lax.broadcasted_iota(jnp.int32, (slots, slots), 0)
    allowed = (across == jnp.transpose(across)) & ((column < count_ref[0]) | (column == row))
    total_out = None
    for head in range(mixed.shape[1] // (3 * VHD)):
        at = head * 3 * VHD
        query = mixed[:, at : at + VHD]
        key = mixed[:, at + VHD : at + 2 * VHD]
        value = mixed[:, at + 2 * VHD : at + 3 * VHD]
        scores = lax.dot_general(
            query, key, (((1,), (1,)), ((), ())), preferred_element_type=jnp.float32
        ) * (1.0 / math.sqrt(VHD))
        scores = jnp.where(allowed, scores, MASKED)
        weights = jnp.exp(scores - jnp.max(scores, axis=-1, keepdims=True))
        total = jnp.sum(weights, axis=-1, keepdims=True)
        result = jnp.dot(weights.astype(jnp.bfloat16), value, preferred_element_type=jnp.float32)
        attended = (result / total).astype(jnp.bfloat16)
        product = jnp.dot(
            attended,
            proj_ref[head * VHD : (head + 1) * VHD, :],
            preferred_element_type=jnp.float32,
        )
        total_out = product if total_out is None else total_out + product
    out_ref[...] = total_out


def merge_kernel(place_ref, patch_ref, part_ref, other_ref, bias_ref, gain_ref, out_ref, share_ref):
    share = share_ref.shape[0]
    whole = patch_ref[...].astype(jnp.float32) + (part_ref[...] + other_ref[...]) + bias_ref[...]
    factor = lax.rsqrt(jnp.mean(whole * whole, axis=-1, keepdims=True) + EPSILON)
    merged = (whole * factor * gain_ref[...]).astype(jnp.bfloat16)
    out_ref[...] = merged
    at = pl.multiple_of(place_ref[2] * share, share)
    share_ref[...] = out_ref[pl.ds(at, share), :]


def collect_kernel(lanes, place_ref, *rest):
    pieces = rest[: 2 * lanes]
    w_ref, sems = rest[2 * lanes :]
    rows = pieces[0].shape[0]
    copies = []
    for e in range(2):
        for d in range(lanes):
            block = ((place_ref[0] % 2) ^ e) * lanes + (place_ref[1] ^ d)
            copies.append(
                pltpu.make_async_copy(
                    pieces[e * lanes + d],
                    w_ref.at[pl.ds(block * rows, rows), :],
                    sems.at[e * lanes + d],
                )
            )
    for copy in copies:
        copy.start()
    for copy in copies:
        copy.wait()


def add_blocks(blocks, pieces, cols, place_ref, gain_ref, w_ref, total):
    squares = None
    for e, piece in zip(blocks, pieces):
        width = piece.shape[1]
        at = pl.multiple_of((place_ref[3] ^ e) * width, width)
        depth = w_ref.shape[0]
        gain_at = pl.multiple_of((place_ref[0] // 2) * depth + at, width)
        rows = piece[...].astype(jnp.float32)
        more = jnp.sum(rows * rows, axis=-1, keepdims=True)
        squares = more if squares is None else squares + more
        scaled = (rows * gain_ref[:, pl.ds(gain_at, width)]).astype(jnp.bfloat16)
        product = jnp.dot(
            scaled, w_ref[pl.ds(at, width), cols], preferred_element_type=jnp.float32
        )
        total = product if total is None else total + product
    return total, squares


def partial_kernel(blocks, place_ref, gain_ref, w_ref, *rest):
    pieces = rest[: len(blocks)]
    sum_ref, square_ref = rest[len(blocks) :]
    total, squares = add_blocks(
        blocks, pieces, slice(0, w_ref.shape[1]), place_ref, gain_ref, w_ref, None
    )
    sum_ref[...] = total
    square_ref[...] = jnp.broadcast_to(squares, square_ref.shape)


def send_keys_kernel(blocks, place_ref, gain_ref, w_ref, *rest):
    pieces = rest[: len(blocks)]
    sum_ref, square_ref, out_ref, all_ref, row_ref = rest[len(blocks) :]
    cols = slice(QH * HD, w_ref.shape[1])
    total, squares = add_blocks(
        blocks, pieces, cols, place_ref, gain_ref, w_ref, sum_ref[:, cols]
    )
    out_ref[...] = total.astype(jnp.bfloat16)
    squares = square_ref[...] + jnp.broadcast_to(squares, square_ref.shape)
    all_ref[...] = squares
    row_ref[...] = jnp.transpose(squares)[: row_ref.shape[0], :]


def send_queries_kernel(blocks, place_ref, gain_ref, w_ref, *rest):
    pieces = rest[: len(blocks)]
    sum_ref, far_ref, near_ref, whole = rest[len(blocks) :]
    cols = slice(0, QH * HD)
    total, _ = add_blocks(blocks, pieces, cols, place_ref, gain_ref, w_ref, sum_ref[:, cols])
    whole[...] = total.astype(jnp.bfloat16)
    rows = far_ref.shape[0]
    half = place_ref[0] // 2
    far_ref[...] = whole[pl.ds(pl.multiple_of(half * rows, rows), rows), :]
    near_ref[...] = whole[pl.ds(pl.multiple_of((1 - half) * rows, rows), rows), :]


def keep_kernel(blocks, place_ref, gain_ref, w_ref, *rest):
    pieces = rest[: len(blocks)]
    out_ref = rest[len(blocks)]
    cols = slice(0, w_ref.shape[1])
    out_ref[...] = add_blocks(blocks, pieces, cols, place_ref, gain_ref, w_ref, None)[0]


def row_factor(depth, all_ref, row_ref):
    rows = jnp.broadcast_to(row_ref[:1, :], (all_ref.shape[1], row_ref.shape[1]))
    squares = all_ref[...] + jnp.transpose(rows)
    return lax.rsqrt(squares / depth + EPSILON)


def turn(x, cosine, sine):
    return x * cosine + pltpu.roll(x, x.shape[1] // 2, 1) * sine


def key_kernel(depth, bias_ref, cos_ref, sin_ref, place_ref, all_ref, row_ref, *rest):
    keep_ref, got_ref, kv_ref = rest
    factor = row_factor(depth, all_ref, row_ref)
    group = keep_ref.shape[1]
    at = pl.multiple_of(place_ref[0] * group + QH * HD, HD)
    total = keep_ref[:, QH * HD :] + got_ref[...].astype(jnp.float32)
    key = total[:, :HD] * factor + bias_ref[:, pl.ds(at, HD)]
    value = total[:, HD:] * factor + bias_ref[:, pl.ds(at + HD, HD)]
    kv_ref[:, :HD] = turn(key, cos_ref[...], sin_ref[...]).astype(jnp.bfloat16)
    kv_ref[:, HD:] = value.astype(jnp.bfloat16)


def query_kernel(depth, far, bias_ref, cos_ref, sin_ref, place_ref, all_ref, row_ref, *rest):
    keep_ref, got_ref, q_ref, factors = rest
    lines, _, _ = q_ref.shape
    rows = got_ref.shape[0]
    tokens = rows // lines
    factors[...] = row_factor(depth, all_ref, row_ref)
    half = place_ref[0] // 2
    half = 1 - half if far else half
    mine = pl.ds(pl.multiple_of(half * rows, rows), rows)
    factor = factors[mine, :]
    cosine = cos_ref[mine, :]
    sine = sin_ref[mine, :]
    group = keep_ref.shape[1]
    for j in range(QH):
        cols = slice(j * HD, (j + 1) * HD)
        at = pl.multiple_of(place_ref[0] * group + j * HD, HD)
        total = keep_ref[mine, cols] + got_ref[:, cols].astype(jnp.float32)
        head = turn(total * factor + bias_ref[:, pl.ds(at, HD)], cosine, sine)
        head = head.astype(jnp.bfloat16)
        for s in range(lines):
            q_ref[s, j * tokens : (j + 1) * tokens, :] = head[s * tokens : (s + 1) * tokens, :]


def gather_kernel(lines, lanes, place_ref, *rest):
    pieces = rest[:lanes]
    kv_ref = rest[lanes]
    tokens = kv_ref.shape[0] // (lines * lanes)
    for d in range(lanes):
        for z in range(lines):
            at = pl.multiple_of((z * lanes + (place_ref[1] ^ d)) * tokens, tokens)
            kv_ref[pl.ds(at, tokens), :] = pieces[d][z * tokens : (z + 1) * tokens, :]


def attend_kernel(which, lanes, place_ref, kv, q_ref, *outs):
    tokens = outs[0].shape[0]
    lane = place_ref[1]
    span = lanes * tokens
    scale = 1.0 / math.sqrt(HD)
    rows = QH * tokens
    row_pos = lane * tokens + lax.rem(lax.broadcasted_iota(jnp.int32, (rows, span), 0), tokens)
    visible = lax.broadcasted_iota(jnp.int32, (rows, span), 1) <= row_pos

    for o_ref, s in zip(outs, which):
        query = q_ref[(place_ref[0] ^ s) % q_ref.shape[0]]

        def visit(chunk, state, masked):
            top, total, summed = state
            at = pl.multiple_of(chunk * span, span)
            key = kv[pl.ds(at, span), :HD]
            value = kv[pl.ds(at, span), HD:]
            scores = (
                lax.dot_general(
                    query, key, (((1,), (1,)), ((), ())), preferred_element_type=jnp.float32
                )
                * scale
            )
            if masked:
                scores = jnp.where(visible, scores, MASKED)
            new_top = jnp.maximum(top, jnp.max(scores, axis=-1, keepdims=True))
            weights = jnp.exp(scores - new_top)
            factor = jnp.exp(top - new_top)
            total = total * factor + jnp.sum(weights, axis=-1, keepdims=True)
            summed = summed * factor + jnp.dot(
                weights.astype(jnp.bfloat16), value, preferred_element_type=jnp.float32
            )
            return new_top, total, summed

        line = place_ref[0] ^ s
        state = (
            jnp.full((rows, 1), MASKED, jnp.float32),
            jnp.zeros((rows, 1), jnp.float32),
            jnp.zeros((rows, HD), jnp.float32),
        )
        state = visit(line, state, True)
        state = lax.fori_loop(0, line, lambda c, st: visit(c, st, False), state)
        _, total, summed = state
        result = (summed / total).astype(jnp.bfloat16)
        for j in range(QH):
            o_ref[:, j * HD : (j + 1) * HD] = result[j * tokens : (j + 1) * tokens, :]


def place_kernel(lines, place_ref, *rest):
    pieces = rest[:lines]
    o_ref = rest[lines]
    width = pieces[0].shape[1]
    for s in range(lines):
        at = pl.multiple_of((place_ref[0] ^ s) * width, width)
        o_ref[:, pl.ds(at, width)] = pieces[s][...]


def grant(mebibytes):
    return pltpu.CompilerParams(vmem_limit_bytes=mebibytes * 2**20)


def on_chip(shape, dtype):
    return pltpu.VMEM(shape, dtype)


def near_core(x):
    return pltpu.with_memory_space_constraint(x, pltpu.VMEM)


def far_core(x):
    return pltpu.with_memory_space_constraint(x, pltpu.HBM)


def ordered(x, *before):
    return lax.optimization_barrier((x,) + before)[0]


def plane_body(lines, lanes):
    size = lines * lanes

    def hop(x, mask):
        return lax.ppermute(x, "ctx", [(c, c ^ mask) for c in range(size)])

    def swap(x):
        return lax.ppermute(x, "head", [(0, 1), (1, 0)])

    def spread(x, r):
        pairs = []
        for c in range(size):
            for h in range(2):
                block = (c // lanes) ^ r
                to = (2 * h + block // 2) * lanes + c % lanes
                pairs.append((2 * c + h, 2 * to + block % 2))
        return lax.ppermute(x, ("ctx", "head"), pairs)

    def plane_gather(pieces):
        one = [hop(p, 1) for p in pieces]
        two = [hop(p, 2) for p in pieces]
        three = []
        for s in range(len(pieces)):
            source, mask = (one[s], 2) if s % 2 == 0 else (two[s], 1)
            three.append(hop(source, mask))
        return (pieces, one, two, three)

    def inner(
        patches,
        patch_count,
        token_patch,
        window_ids,
        text_embed,
        vit_norm_gain,
        vit_qkv,
        vit_qkv_bias,
        vit_proj,
        vit_proj_bias,
        merge_norm_gain,
        merger,
        merger_bias,
        llm_norm_gain,
        w_qkv,
        qkv_bias,
    ):
        ctx_index = lax.axis_index("ctx")
        line = ctx_index // lanes
        lane = ctx_index % lanes
        side = lax.axis_index("head")
        tokens = patches.shape[0]
        own_cols = text_embed.shape[1]
        group_cols = (QH + 2) * HD
        mine = 2 * (line % 2) + side
        places = jnp.stack([line, lane, side, mine]).astype(jnp.int32)
        part_cols = own_cols // lines

        cut = pl.pallas_call(
            lambda *refs: cut_kernel(group_cols, *refs),
            out_shape=[on_chip((w_qkv.shape[0], group_cols), jnp.bfloat16)] * lines,
            in_specs=[smem_spec(), vmem_spec()],
            out_specs=[vmem_spec()] * lines,
            compiler_params=grant(8),
            name="cut",
        )(places, far_core(w_qkv))
        far_all = plane_gather([cut[0], hop(cut[2], lanes)])
        own_all = plane_gather([cut[1], hop(cut[3], lanes)])

        packed = pl.pallas_call(
            pack_kernel,
            out_shape=[on_chip((tokens + merger.shape[0] + 16, part_cols), jnp.bfloat16)] * lines,
            in_specs=[smem_spec()] + [vmem_spec()] * 4,
            out_specs=[vmem_spec()] * lines,
            compiler_params=grant(8),
            name="pack",
        )(
            places,
            far_core(text_embed),
            far_core(merger),
            far_core(token_patch.reshape(1, -1)),
            far_core(merger_bias.reshape(1, -1)),
        )
        packed = [spread(x, r) for r, x in enumerate(packed)]
        span = slice(tokens, tokens + merger.shape[0])
        merger_own = jnp.concatenate([p[span] for p in packed], axis=0)
        merger_all = [merger_own] + [hop(merger_own, d) for d in range(1, lanes)]

        width = patches.shape[1]
        part = pl.pallas_call(
            vision_kernel,
            out_shape=on_chip((tokens, width), jnp.float32),
            in_specs=[smem_spec()] + [vmem_spec()] * 6,
            out_specs=vmem_spec(),
            compiler_params=grant(24),
            name="vision",
        )(
            patch_count,
            far_core(patches),
            far_core(vit_norm_gain),
            far_core(vit_qkv),
            far_core(vit_qkv_bias),
            far_core(window_ids.reshape(1, -1)),
            near_core(vit_proj),
        )
        other_part = swap(part)
        merged_in, merged_share = pl.pallas_call(
            merge_kernel,
            out_shape=[
                on_chip((tokens, width), jnp.bfloat16),
                on_chip((tokens // 2, width), jnp.bfloat16),
            ],
            in_specs=[smem_spec()] + [vmem_spec()] * 5,
            out_specs=[vmem_spec()] * 2,
            compiler_params=grant(12),
            name="merge",
        )(
            places,
            patches,
            part,
            other_part,
            vit_proj_bias.reshape(1, -1),
            merge_norm_gain.reshape(1, -1),
        )
        near = jnp.concatenate([hop(merged_share, s * lanes) for s in range(1, lines)], axis=0)
        far = swap(near)

        stitched = pl.pallas_call(
            lambda *refs: image_kernel(lines, lanes, *refs),
            out_shape=on_chip((lines * tokens, part_cols), jnp.bfloat16),
            in_specs=[smem_spec()] + [vmem_spec()] * (3 + lines + lanes),
            out_specs=vmem_spec(),
            scratch_shapes=[
                pltpu.VMEM((lines * tokens, merged_in.shape[1]), jnp.bfloat16),
                pltpu.VMEM((merger.shape[0] * size, part_cols), jnp.bfloat16),
            ],
            compiler_params=grant(24),
            name="image",
        )(places, merged_in, near, far, *packed, *merger_all)

        beside = swap(stitched)
        across = hop(stitched, lanes)
        both = swap(across)

        late = ordered(ctx_index, stitched)
        half = HD // 2
        steps = jnp.arange(half, dtype=jnp.float32) * (2.0 / HD)
        frequency = jnp.exp(-math.log(THETA) * steps)
        row = jnp.arange(lines * tokens, dtype=jnp.int32)
        positions = ((row // tokens) * lanes + late % lanes) * tokens
        positions = positions + row % tokens
        angle = positions.astype(jnp.float32)[:, None] * frequency[None, :]
        cosine = jnp.cos(angle)
        sine = jnp.sin(angle)
        cosine = jnp.concatenate([cosine, cosine], axis=-1)
        sine = jnp.concatenate([-sine, sine], axis=-1)

        gain = llm_norm_gain.reshape(1, -1)
        bias = qkv_bias.reshape(1, -1)
        depth = w_qkv.shape[0] * size
        rows = lines * tokens

        def collect(pieces):
            return pl.pallas_call(
                lambda *refs: collect_kernel(lanes, *refs),
                out_shape=on_chip((depth // 2, group_cols), jnp.bfloat16),
                in_specs=[smem_spec()] + [any_spec()] * (2 * lanes),
                out_specs=vmem_spec(),
                scratch_shapes=[pltpu.SemaphoreType.DMA((2 * lanes,))],
                compiler_params=grant(16),
                name="collect",
            )(places, *[pieces[d][e] for e in range(2) for d in range(lanes)])

        def product(kernel, weight, shapes, *operands, scratch=()):
            return pl.pallas_call(
                kernel,
                out_shape=shapes,
                in_specs=[smem_spec()] + [vmem_spec()] * (2 + len(operands)),
                out_specs=[vmem_spec()] * len(shapes),
                scratch_shapes=list(scratch),
                compiler_params=grant(28),
            )(places, gain, weight, *operands)

        far_weight = collect(far_all)
        own_weight = collect(own_all)
        sums, squares = product(
            lambda *refs: partial_kernel((0, 1), *refs),
            far_weight,
            [on_chip((rows, group_cols), jnp.float32), on_chip((rows, HD), jnp.float32)],
            stitched,
            beside,
        )
        last = (2, 3)
        send_kv, all_squares, square_row = product(
            lambda *refs: send_keys_kernel(last, *refs),
            far_weight,
            [
                on_chip((rows, 2 * HD), jnp.bfloat16),
                on_chip((rows, HD), jnp.float32),
                on_chip((8, rows), jnp.float32),
            ],
            across,
            both,
            sums,
            squares,
        )
        got_kv = hop(send_kv, 2 * lanes)
        got_row = hop(square_row, 2 * lanes)
        send_far, send_near = product(
            lambda *refs: send_queries_kernel(last, *refs),
            far_weight,
            [on_chip((rows // 2, QH * HD), jnp.bfloat16)] * 2,
            across,
            both,
            sums,
            scratch=[pltpu.VMEM((rows, QH * HD), jnp.bfloat16)],
        )
        got_far = hop(send_far, 2 * lanes)
        got_near = hop(send_near, 2 * lanes)
        (kept,) = product(
            lambda *refs: keep_kernel((0, 1, 2, 3), *refs),
            own_weight,
            [on_chip((rows, group_cols), jnp.float32)],
            stitched,
            beside,
            across,
            both,
        )
        closing = (bias, cosine, sine, places, all_squares, got_row, kept)
        closing_specs = [vmem_spec()] * 3 + [smem_spec()] + [vmem_spec()] * 4
        kv = pl.pallas_call(
            lambda *refs: key_kernel(depth, *refs),
            out_shape=on_chip((rows, 2 * HD), jnp.bfloat16),
            in_specs=closing_specs,
            out_specs=vmem_spec(),
            compiler_params=grant(24),
            name="keys",
        )(*closing, got_kv)
        kv_pieces = [kv] + [hop(kv, d) for d in range(1, lanes)]

        def queries_of(far, got):
            return pl.pallas_call(
                lambda *refs: query_kernel(depth, far, *refs),
                out_shape=on_chip((lines // 2, QH * tokens, HD), jnp.bfloat16),
                in_specs=closing_specs,
                out_specs=vmem_spec(),
                scratch_shapes=[pltpu.VMEM((rows, HD), jnp.float32)],
                compiler_params=grant(24),
                name="queries",
            )(*closing, got)

        query_far = queries_of(True, got_far)
        kv_all = pl.pallas_call(
            lambda *refs: gather_kernel(lines, lanes, *refs),
            out_shape=on_chip((size * tokens, 2 * HD), jnp.bfloat16),
            in_specs=[smem_spec()] + [vmem_spec()] * lanes,
            out_specs=vmem_spec(),
            compiler_params=grant(8),
            name="gather",
        )(places, *kv_pieces)

        def attend(which, kv_all, query):
            return pl.pallas_call(
                lambda *refs: attend_kernel(which, lanes, *refs),
                out_shape=[on_chip((tokens, QH * HD), jnp.bfloat16)] * len(which),
                in_specs=[smem_spec()] + [vmem_spec()] * 2,
                out_specs=[vmem_spec()] * len(which),
                compiler_params=grant(24),
                name="attend",
            )(places, kv_all, query)

        three, two = attend((3, 2), kv_all, query_far)
        query_near = queries_of(False, ordered(got_near, three))
        (one,) = attend((1,), kv_all, query_near)
        (own,) = attend((0,), ordered(kv_all, one), query_near)
        three = hop(three, 3 * lanes)
        two = hop(two, 2 * lanes)
        one = hop(one, lanes)
        return pl.pallas_call(
            lambda *refs: place_kernel(lines, *refs),
            out_shape=jax.ShapeDtypeStruct((tokens, lines * QH * HD), jnp.bfloat16),
            in_specs=[smem_spec()] + [vmem_spec()] * lines,
            out_specs=vmem_spec(),
            compiler_params=grant(8),
            name="place",
        )(places, *[near_core(x) for x in (own, one, two, three)])

    return inner


def solution(mesh):
    specs = (
        P("ctx", None),
        P("ctx"),
        P("ctx"),
        P("ctx"),
        P("ctx", "head"),
        P(),
        P(None, "head"),
        P("head"),
        P("head", None),
        P(),
        P(),
        P("ctx", "head"),
        P("head"),
        P(),
        P("ctx", "head"),
        P("head"),
    )
    lines = KVH // mesh.shape["head"]
    lanes = mesh.shape["ctx"] // lines
    planes = mesh.shape["head"] == 2 and lines == 4 and lanes == 4
    body = plane_body(lines, lanes) if planes else general_body
    return jax.shard_map(
        body, mesh=mesh, in_specs=specs, out_specs=P("ctx", "head"), check_vma=False
    )
```
